32 devices in a mesh: tp: 4 (over y, core), dp: 8 (over z, x).
Axes of the slice: x: 2, y: 2, z: 4, core: 2. Of those that a mesh axis runs over, the one named last changes fastest.
Arguments:
- teacher_query: bfloat16 [8192, 8192], P('dp', 'tp'), may hold values from -8 to 8
- student_hidden: bfloat16 [8192, 4096], P('dp', 'tp'), may hold values from -16 to 16
- query_weight: bfloat16 [4096, 4096], P('dp', 'tp'), may hold values from -0.039794922 to 0.039794922
Outputs:
- kl_rows: float32 [32, 8192], P(('tp', 'dp'))
- weight_grad: float32 [4096, 4096], P('dp', 'tp')
The draws below stay inside these ranges and needn't reach their ends.
All inputs are finite; a program needn't handle non-finite values.
Results may differ from the reference program's by a relative error of at most 0.0029.
Values may be sent and summed in bfloat16 or wider, within the bound.
A program may use at most 64 MiB of HBM per device.

```python
import jax
import jax.numpy as jnp
from jax import lax

DT = 8192
DS = 4096
RHEADS = 32
NSEQ = 2
SEQ = 4096
QBLOCKS = 1
QROWS = 4096


def draw_teacher_query(key, part):
    values = 0.5 * jnp.clip(jax.random.normal(jax.random.fold_in(key, 1), (NSEQ * SEQ, DT), jnp.float32), -4.0, 4.0)
    return values.astype(jnp.bfloat16)


def draw_student_hidden(key, part):
    values = jnp.clip(jax.random.normal(jax.random.fold_in(key, 2), (NSEQ * SEQ, DS), jnp.float32), -4.0, 4.0)
    return values.astype(jnp.bfloat16)


def steps_of(rng, dims, cuts, smallest, largest):
    def one(position, parts):
        heights = jax.random.uniform(jax.random.fold_in(jax.random.fold_in(rng, 6), position), (parts,), jnp.float32, smallest / len(cuts), largest / len(cuts))
        return jnp.repeat(jnp.exp(heights), dims[position] // parts).reshape((-1,) + (1,) * (len(dims) - position - 1))

    factor_of = one(*cuts[0])
    for cut in cuts[1:]:
        factor_of = factor_of * one(*cut)
    return factor_of


def noise(stream_key, shape, scale, bound, shards=(), held_as=jnp.bfloat16):
    drawn = jax.random.normal(stream_key, shape, jnp.float32) * scale
    if len(shards) > 0:
        drawn = steps_of(stream_key, shape, shards, -0.22, 0.18) * drawn
    return jnp.clip(drawn, min=-bound, max=bound).astype(held_as)


def setup_inputs(seed: int = 0) -> dict:
    arg_keys = jax.random.split(jax.random.key(seed), 4)
    return {
        "teacher_query": draw_teacher_query(jax.random.fold_in(arg_keys[3], 71), 0),
        "student_hidden": draw_student_hidden(jax.random.fold_in(arg_keys[3], 71), 0),
        "query_weight": noise(arg_keys[2], (DS, DS), 0.0078125, 0.039794922, ((0, 8), (1, 4))),
    }


def head_terms(pair):
    teacher_head, student_head = pair
    teacher_scale = teacher_head.shape[1] ** -0.5
    student_scale = student_head.shape[1] ** -0.5
    teacher_scores = lax.dot_general(teacher_head, teacher_head, (((1,), (1,)), ((), ())), preferred_element_type=jnp.float32) * teacher_scale
    student_scores = lax.dot_general(student_head, student_head, (((1,), (1,)), ((), ())), preferred_element_type=jnp.float32) * student_scale
    teacher_log = jax.nn.log_softmax(teacher_scores, axis=-1)
    student_log = jax.nn.log_softmax(student_scores, axis=-1)
    teacher_prob = jnp.exp(teacher_log)
    divergence = jnp.sum(teacher_prob * (teacher_log - student_log), axis=-1)
    score_grad = (jnp.exp(student_log) - teacher_prob).astype(jnp.bfloat16)
    row_part = jnp.dot(score_grad, student_head, preferred_element_type=jnp.float32)
    key_part = lax.dot_general(score_grad, student_head, (((0,), (0,)), ((), ())), preferred_element_type=jnp.float32)
    return divergence, (row_part + key_part) * student_scale


def reference(teacher_query, student_hidden, query_weight):
    student_query = jnp.dot(student_hidden, query_weight, preferred_element_type=jnp.float32).astype(jnp.bfloat16)
    teacher_width = DT // RHEADS
    student_width = DS // RHEADS
    teacher_heads = teacher_query.reshape(NSEQ, SEQ, RHEADS, teacher_width).transpose(2, 0, 1, 3).reshape(RHEADS * NSEQ, SEQ, teacher_width)
    student_heads = student_query.reshape(NSEQ, SEQ, RHEADS, student_width).transpose(2, 0, 1, 3).reshape(RHEADS * NSEQ, SEQ, student_width)
    divergence, head_grads = lax.map(head_terms, (teacher_heads, student_heads))
    query_grad = head_grads.reshape(RHEADS, NSEQ, SEQ, student_width).transpose(1, 2, 0, 3).reshape(NSEQ * SEQ, DS).astype(jnp.bfloat16)
    weight_grad = lax.dot_general(student_hidden, query_grad, (((0,), (0,)), ((), ())), preferred_element_type=jnp.float32)
    kl_rows = divergence.reshape(RHEADS, NSEQ, QBLOCKS, QROWS).transpose(0, 2, 1, 3).reshape(RHEADS * QBLOCKS, NSEQ * QROWS)
    return kl_rows, weight_grad
```

```python
import functools
import math

import jax
import jax.numpy as jnp
from jax import lax
from jax.experimental import pallas as pl
from jax.experimental.pallas import tpu as pltpu
from jax.sharding import PartitionSpec as P

RHEADS = 32
NSEQ = 2
SEQ = 4096


def spread_heads(queries, heads, copies):
    rows = queries.shape[0]
    width = queries.shape[1] // heads
    shaped = queries.reshape(rows, heads, 1, width)
    return jnp.broadcast_to(shaped, (rows, heads, copies, width)).reshape(
        rows, heads * copies, width
    )

LOG2E = 1.0 / math.log(2.0)
LN2 = math.log(2.0)
LANES = 128


def relation_body(
    t_rows, t_keys, s_rows, s_keys, s_rows_t, kl_out, grad_out, t_buf, s_buf, g_buf, row_acc, key_acc,
    *, group, chunk, t_scale, s_scale,
):
    step = pl.program_id(0)
    block = t_rows.shape[0]
    keys = t_keys.shape[0]
    nt = (((1,), (1,)), ((), ()))

    for c in range(keys // chunk):
        at = slice(c * chunk, (c + 1) * chunk)
        t_buf[:, at] = lax.dot_general(t_rows[...], t_keys[at, :], nt, preferred_element_type=jnp.float32)
        s_buf[:, at] = lax.dot_general(s_rows[...], s_keys[at, :], nt, preferred_element_type=jnp.float32)

    tiles = keys // LANES
    ct = t_scale * LOG2E
    cs = s_scale * LOG2E

    def rows_of(i, carry):
        at = pl.ds(pl.multiple_of(i * group, group), group)
        t_max = t_buf[at, 0:LANES]
        s_max = s_buf[at, 0:LANES]
        for k in range(1, tiles):
            cols = slice(k * LANES, (k + 1) * LANES)
            t_max = jnp.maximum(t_max, t_buf[at, cols])
            s_max = jnp.maximum(s_max, s_buf[at, cols])
        t_max = jnp.broadcast_to(jnp.max(t_max, axis=1, keepdims=True), (group, LANES))
        s_max = jnp.broadcast_to(jnp.max(s_max, axis=1, keepdims=True), (group, LANES))
        t_sum = jnp.zeros((group, LANES), jnp.float32)
        s_sum = jnp.zeros((group, LANES), jnp.float32)
        gap = jnp.zeros((group, LANES), jnp.float32)
        for k in range(tiles):
            cols = slice(k * LANES, (k + 1) * LANES)
            u = (t_buf[at, cols] - t_max) * ct
            v = (s_buf[at, cols] - s_max) * cs
            t_exp = jnp.exp2(u)
            s_exp = jnp.exp2(v)
            t_buf[at, cols] = t_exp
            s_buf[at, cols] = s_exp
            t_sum = t_sum + t_exp
            s_sum = s_sum + s_exp
            gap = gap + t_exp * (u - v)
        t_sum = jnp.sum(t_sum, axis=1, keepdims=True)
        s_sum = jnp.sum(s_sum, axis=1, keepdims=True)
        gap = jnp.sum(gap, axis=1, keepdims=True)
        kl = gap * LN2 / t_sum - jnp.log(t_sum) + jnp.log(s_sum)
        kl_out[0, at, :] = jnp.broadcast_to(kl, (group, LANES))
        t_inv = jnp.broadcast_to(1.0 / t_sum, (group, LANES))
        s_inv = jnp.broadcast_to(1.0 / s_sum, (group, LANES))
        for k in range(tiles):
            cols = slice(k * LANES, (k + 1) * LANES)
            g_buf[at, cols] = (s_buf[at, cols] * s_inv - t_buf[at, cols] * t_inv).astype(jnp.bfloat16)
        return carry

    lax.fori_loop(0, block // group, rows_of, 0)

    @pl.when(step == 0)
    def _():
        key_acc[...] = jnp.zeros_like(key_acc)

    row_acc[pl.ds(pl.multiple_of(step * block, block), block), :] = jnp.dot(
        g_buf[...], s_keys[...], preferred_element_type=jnp.float32
    )
    for c in range(keys // chunk):
        at = slice(c * chunk, (c + 1) * chunk)
        key_acc[:, at] += jnp.dot(s_rows_t[...], g_buf[:, at], preferred_element_type=jnp.float32)

    @pl.when(step == pl.num_programs(0) - 1)
    def _():
        def finish(c, carry):
            at = pl.ds(pl.multiple_of(c * LANES, LANES), LANES)
            grad_out[at, :] = ((row_acc[at, :] + key_acc[:, at].T) * s_scale).astype(jnp.bfloat16)
            return carry

        lax.fori_loop(0, keys // LANES, finish, 0)


def relation(teacher, student, part, parts):
    keys = teacher.shape[0]
    t_width = teacher.shape[1] // parts
    s_width = student.shape[1] // parts
    block = min(256, keys)
    group = 16
    chunk = min(1024, keys)
    steps = keys // block
    kl, grad = pl.pallas_call(
        functools.partial(
            relation_body, group=group, chunk=chunk, t_scale=t_width ** (-0.5), s_scale=s_width ** (-0.5)
        ),
        grid=(steps,),
        in_specs=[
            pl.BlockSpec((block, t_width), lambda i: (i, part)),
            pl.BlockSpec((keys, t_width), lambda i: (0, part)),
            pl.BlockSpec((block, s_width), lambda i: (i, part)),
            pl.BlockSpec((keys, s_width), lambda i: (0, part)),
            pl.BlockSpec((s_width, block), lambda i: (part, i)),
        ],
        out_specs=[
            pl.BlockSpec((1, block, LANES), lambda i: (i, 0, 0)),
            pl.BlockSpec((keys, s_width), lambda i: (0, 0)),
        ],
        out_shape=[
            jax.ShapeDtypeStruct((steps, block, LANES), jnp.float32),
            jax.ShapeDtypeStruct((keys, s_width), jnp.bfloat16),
        ],
        scratch_shapes=[
            pltpu.VMEM((block, keys), jnp.float32),
            pltpu.VMEM((block, keys), jnp.float32),
            pltpu.VMEM((block, keys), jnp.bfloat16),
            pltpu.VMEM((keys, s_width), jnp.float32),
            pltpu.VMEM((s_width, keys), jnp.float32),
        ],
        compiler_params=pltpu.CompilerParams(
            dimension_semantics=("arbitrary",), vmem_limit_bytes=40 * 1024 * 1024
        ),
        name="relation",
    )(teacher, teacher, student, student, student.T)
    return kl[:, :, 0].reshape(keys), grad


def heads_of_one_sequence(teacher_query, student_hidden, query_weight):
    members = lax.axis_size("dp") // NSEQ
    mine = RHEADS // lax.axis_size("tp") // members
    groups = [[s * members + k for k in range(members)] for s in range(NSEQ)]
    to_heads = functools.partial(
        lax.all_to_all, axis_name="dp", split_axis=1, concat_axis=0, axis_index_groups=groups, tiled=True
    )
    teacher_all = to_heads(teacher_query)
    hidden_full = lax.all_gather(student_hidden, "tp", axis=1, tiled=True)
    weight_full = lax.all_gather(query_weight, "dp", axis=0, tiled=True)
    student_query = jnp.dot(hidden_full, weight_full, preferred_element_type=jnp.float32).astype(jnp.bfloat16)
    student_all = to_heads(student_query)
    rows_of = [0.0] * NSEQ
    grads = []
    for m in range(mine):
        kl, grad = relation(teacher_all, student_all, m, mine)
        for s in range(NSEQ):
            pairs = [(s * members + k, k * mine + m) for k in range(members)]
            rows_of[s] = rows_of[s] + lax.ppermute(kl, "dp", pairs)
        part = lax.all_to_all(
            grad, "dp", split_axis=0, concat_axis=1, axis_index_groups=groups, tiled=True
        )
        grads.append(part.reshape(part.shape[0], members, 1, part.shape[1] // members))
    grad_rows = jnp.concatenate(grads, axis=2).reshape(student_query.shape)
    partial = lax.dot_general(
        hidden_full, grad_rows, (((0,), (0,)), ((), ())), preferred_element_type=jnp.float32
    )
    size = lax.axis_size("dp")
    pieces = partial.reshape(size, partial.shape[0] // size, partial.shape[1]).astype(jnp.bfloat16)
    landed = lax.all_to_all(pieces, "dp", split_axis=0, concat_axis=0, tiled=True)
    return jnp.concatenate(rows_of).reshape(1, NSEQ * SEQ), jnp.sum(landed.astype(jnp.float32), axis=0)


def local(teacher_query, student_hidden, query_weight):
    heads_here = RHEADS // lax.axis_size("tp")
    copies = lax.axis_size("dp") // heads_here
    if lax.axis_size("dp") % NSEQ == 0 and heads_here % (lax.axis_size("dp") // NSEQ) == 0:
        return heads_of_one_sequence(teacher_query, student_hidden, query_weight)
    rows = teacher_query.shape[0]
    teacher_width = teacher_query.shape[1] // heads_here
    hidden_full = lax.all_gather(student_hidden, "tp", axis=1, tiled=True)
    teacher_send = spread_heads(teacher_query, heads_here, copies)
    projected = jnp.dot(
        hidden_full,
        lax.all_gather(query_weight, "dp", axis=0, tiled=True),
        preferred_element_type=jnp.float32,
    )
    student_query = projected.astype(jnp.bfloat16)
    student_width = student_query.shape[1] // heads_here
    student_send = spread_heads(student_query, heads_here, copies)
    teacher_all, student_all = (
        lax.all_to_all(teacher_send, "dp", split_axis=1, concat_axis=0, tiled=True),
        lax.all_to_all(student_send, "dp", split_axis=1, concat_axis=0, tiled=True),
    )
    total_rows = teacher_all.shape[0]
    teacher_all = teacher_all.reshape(total_rows, teacher_width)
    student_all = student_all.reshape(total_rows, student_width)
    teacher_scale = teacher_width ** (-0.5)
    student_scale = student_width ** (-0.5)
    query_rows = SEQ // copies
    first_row = lax.axis_index("dp") % copies * query_rows
    block = min(512, query_rows)
    blocks_each = query_rows // block

    def relation_step(step, carry):
        kl_store, grad_store = carry
        sequence = step // blocks_each
        offset = step % blocks_each * block
        base = sequence * SEQ
        start = base + first_row + offset
        teacher_keys = lax.dynamic_slice_in_dim(teacher_all, base, SEQ, 0)
        student_keys = lax.dynamic_slice_in_dim(student_all, base, SEQ, 0)
        teacher_rows = lax.dynamic_slice_in_dim(teacher_all, start, block, 0)
        student_rows = lax.dynamic_slice_in_dim(student_all, start, block, 0)
        teacher_scores = (
            lax.dot_general(
                teacher_rows,
                teacher_keys,
                (((1,), (1,)), ((), ())),
                preferred_element_type=jnp.float32,
            )
            * teacher_scale
        )
        student_scores = (
            lax.dot_general(
                student_rows,
                student_keys,
                (((1,), (1,)), ((), ())),
                preferred_element_type=jnp.float32,
            )
            * student_scale
        )
        teacher_log = jax.nn.log_softmax(teacher_scores, axis=-1)
        student_log = jax.nn.log_softmax(student_scores, axis=-1)
        teacher_prob = jnp.exp(teacher_log)
        divergence = jnp.sum(teacher_prob * (teacher_log - student_log), axis=-1)
        score_grad = (jnp.exp(student_log) - teacher_prob).astype(jnp.bfloat16)
        key_part = (
            lax.dot_general(
                score_grad,
                student_rows,
                (((0,), (0,)), ((), ())),
                preferred_element_type=jnp.float32,
            )
            * student_scale
        )
        row_part = (
            jnp.dot(score_grad, student_keys, preferred_element_type=jnp.float32) * student_scale
        )
        seq_grad = lax.dynamic_slice_in_dim(grad_store, base, SEQ, 0)
        grad_store = lax.dynamic_update_slice_in_dim(grad_store, seq_grad + key_part, base, 0)
        current = lax.dynamic_slice_in_dim(grad_store, start, block, 0)
        grad_store = lax.dynamic_update_slice_in_dim(grad_store, current + row_part, start, 0)
        kl_store = lax.dynamic_update_slice_in_dim(
            kl_store, divergence, sequence * query_rows + offset, 0
        )
        return (kl_store, grad_store)

    kl_init = jnp.zeros((NSEQ * query_rows,), jnp.float32)
    grad_init = jnp.zeros((total_rows, student_width), jnp.float32)
    kl_store, grad_store = lax.fori_loop(0, NSEQ * blocks_each, relation_step, (kl_init, grad_init))
    returned = lax.all_to_all(
        grad_store.reshape(heads_here * copies, rows, student_width),
        "dp",
        split_axis=0,
        concat_axis=2,
        tiled=True,
    )
    summed = jnp.sum(returned.reshape(rows, heads_here, copies, student_width), axis=2)
    query_grad = summed.reshape(rows, heads_here * student_width).astype(jnp.bfloat16)
    weight_grad = lax.psum_scatter(
        lax.dot_general(
            hidden_full, query_grad, (((0,), (0,)), ((), ())), preferred_element_type=jnp.float32
        ),
        "dp",
        scatter_dimension=0,
        tiled=True,
    )
    return (kl_store.reshape(1, NSEQ * query_rows), weight_grad)


def solution(mesh):
    placed = (P("dp", "tp"), P("dp", "tp"), P("dp", "tp"))
    return jax.shard_map(
        local,
        mesh=mesh,
        in_specs=placed,
        out_specs=(P(("tp", "dp"), None), P("dp", "tp")),
        check_vma=False,
    )
```

```python
import functools
import math

import jax
import jax.numpy as jnp
from jax import lax
from jax.experimental import pallas as pl
from jax.experimental.pallas import tpu as pltpu
from jax.sharding import PartitionSpec as P

RHEADS = 32
NSEQ = 2
SEQ = 4096


def spread_heads(queries, heads, copies):
    rows = queries.shape[0]
    width = queries.shape[1] // heads
    shaped = queries.reshape(rows, heads, 1, width)
    return jnp.broadcast_to(shaped, (rows, heads, copies, width)).reshape(
        rows, heads * copies, width
    )

LOG2E = 1.0 / math.log(2.0)
LN2 = math.log(2.0)
LANES = 128


NT = (((1,), (1,)), ((), ()))


def stage(t_keys, s_keys, s_turned, kl_out, t_new, s_new, t_old, s_old, g_new, g_old, exps, row_acc, key_acc,
          *, score_row, grad_row, group, t_scale, s_scale):
    block, keys = t_new.shape
    groups = block // group
    pieces = groups // 2
    chunk = keys // pieces
    tiles = keys // LANES
    ct = t_scale * LOG2E
    cs = s_scale * LOG2E
    rows = pl.ds(pl.multiple_of(score_row, block), block)
    old_rows = pl.ds(pl.multiple_of(grad_row, block), block)

    def rows_at(i):
        return pl.ds(pl.multiple_of(i * group, group), group)

    def tops(i):
        at = rows_at(i)
        t_max = t_old[at, 0:LANES]
        s_max = s_old[at, 0:LANES]
        for k in range(1, tiles):
            c = slice(k * LANES, (k + 1) * LANES)
            t_max = jnp.maximum(t_max, t_old[at, c])
            s_max = jnp.maximum(s_max, s_old[at, c])
        return (
            jnp.broadcast_to(jnp.max(t_max, axis=1, keepdims=True), (group, LANES)),
            jnp.broadcast_to(jnp.max(s_max, axis=1, keepdims=True), (group, LANES)),
        )

    def sums(i, t_max, s_max, t_e, s_e):
        at = rows_at(i)
        t_sum = jnp.zeros((group, LANES), jnp.float32)
        s_sum = jnp.zeros((group, LANES), jnp.float32)
        gap = jnp.zeros((group, LANES), jnp.float32)
        for k in range(tiles):
            c = slice(k * LANES, (k + 1) * LANES)
            u = (t_old[at, c] - t_max) * ct
            v = (s_old[at, c] - s_max) * cs
            t_exp = jnp.exp2(u)
            s_exp = jnp.exp2(v)
            t_e[:, c] = t_exp
            s_e[:, c] = s_exp
            t_sum = t_sum + t_exp
            s_sum = s_sum + s_exp
            gap = gap + t_exp * (u - v)
        t_sum = jnp.sum(t_sum, axis=1, keepdims=True)
        s_sum = jnp.sum(s_sum, axis=1, keepdims=True)
        gap = jnp.sum(gap, axis=1, keepdims=True)
        kl = gap * LN2 / t_sum - jnp.log(t_sum) + jnp.log(s_sum)
        kl_out[0, at, :] = jnp.broadcast_to(kl, (group, LANES))
        return jnp.broadcast_to(1.0 / t_sum, (group, LANES)), jnp.broadcast_to(1.0 / s_sum, (group, LANES))

    def score_grads(i, t_inv, s_inv, t_e, s_e):
        at = rows_at(i)
        for k in range(tiles):
            c = slice(k * LANES, (k + 1) * LANES)
            g_new[at, c] = (s_e[:, c] * s_inv - t_e[:, c] * t_inv).astype(jnp.bfloat16)

    def matmuls(i):
        half = chunk // 2
        for h in range(2):
            cols = pl.ds(pl.multiple_of(i * chunk + h * half, half), half)
            t_new[:, cols] = lax.dot_general(t_keys[rows, :], t_keys[cols, :], NT, preferred_element_type=jnp.float32)
            s_new[:, cols] = lax.dot_general(s_keys[rows, :], s_keys[cols, :], NT, preferred_element_type=jnp.float32)
            key_acc[:, cols] += jnp.dot(s_turned[:, old_rows], g_old[:, cols], preferred_element_type=jnp.float32)
        cols = pl.ds(pl.multiple_of(i * chunk, chunk), chunk)
        row_acc[:, old_rows] += lax.dot_general(
            s_turned[:, cols], g_old[:, cols], NT, preferred_element_type=jnp.float32
        )

    t_even, s_even, t_odd, s_odd = exps

    def work(i, carry):
        even_max, odd_inv = carry
        matmuls(i)
        odd_max = tops(2 * i + 1)
        score_grads(jnp.maximum(2 * i - 1, 0), *odd_inv, t_odd, s_odd)
        even_inv = sums(2 * i, *even_max, t_even, s_even)
        next_max = tops(jnp.minimum(2 * i + 2, groups - 1))
        score_grads(2 * i, *even_inv, t_even, s_even)
        odd_inv = sums(2 * i + 1, *odd_max, t_odd, s_odd)
        return next_max, odd_inv

    zero = jnp.zeros((group, LANES), jnp.float32)
    _, odd_inv = lax.fori_loop(0, pieces, work, (tops(0), (zero, zero)))
    score_grads(groups - 1, *odd_inv, t_odd, s_odd)


def relation_body(t_keys, s_keys, s_turned, kl_out, grad_out,
                  t_a, s_a, g_a, t_b, s_b, g_b, t_even, s_even, t_odd, s_odd, row_acc, key_acc, *, steps, group, t_scale, s_scale):
    step = pl.program_id(0)
    block = t_a.shape[0]
    keys = t_a.shape[1]
    last = pl.num_programs(0) - 3
    score_row = jnp.minimum(step, last) % steps * block
    grad_row = jnp.maximum(step - 2, 0) % steps * block

    @pl.when(jnp.logical_or(step < 2, (step - 2) % steps == 0))
    def _():
        row_acc[...] = jnp.zeros_like(row_acc)
        key_acc[...] = jnp.zeros_like(key_acc)

    for parity, (t_new, s_new, g_new, t_old, s_old, g_old) in enumerate(
        ((t_a, s_a, g_a, t_b, s_b, g_b), (t_b, s_b, g_b, t_a, s_a, g_a))
    ):
        @pl.when(step % 2 == parity)
        def _():
            stage(t_keys, s_keys, s_turned, kl_out, t_new, s_new, t_old, s_old, g_new, g_old,
                  (t_even, s_even, t_odd, s_odd), row_acc, key_acc,
                  score_row=score_row, grad_row=grad_row, group=group, t_scale=t_scale, s_scale=s_scale)

    @pl.when(jnp.logical_and(step >= 2, (step - 2) % steps == steps - 1))
    def _():
        def finish(c, carry):
            at = pl.ds(pl.multiple_of(c * LANES, LANES), LANES)
            grad_out[at, :] = ((row_acc[:, at] + key_acc[:, at]).T * s_scale).astype(jnp.bfloat16)
            return carry
        lax.fori_loop(0, keys // LANES, finish, 0)


def relation(teacher, student, parts):
    keys = teacher.shape[0]
    t_width = teacher.shape[1] // parts
    s_width = student.shape[1] // parts
    block = min(256, keys)
    group = 32
    steps = keys // block
    last = parts * steps - 1
    score_part = lambda i: jnp.minimum(i, last) // steps
    grad_part = lambda i: jnp.maximum(i - 2, 0) // steps
    kl, grad = pl.pallas_call(
        functools.partial(relation_body, steps=steps, group=group, t_scale=t_width ** (-0.5), s_scale=s_width ** (-0.5)),
        grid=(parts * steps + 2,),
        in_specs=[
            pl.BlockSpec((keys, t_width), lambda i: (0, score_part(i))),
            pl.BlockSpec((keys, s_width), lambda i: (0, score_part(i))),
            pl.BlockSpec((s_width, keys), lambda i: (grad_part(i), 0)),
        ],
        out_specs=[
            pl.BlockSpec((1, block, LANES), lambda i: (jnp.clip(i - 1, 0, last), 0, 0)),
            pl.BlockSpec((keys, s_width), lambda i: (0, grad_part(i))),
        ],
        out_shape=[
            jax.ShapeDtypeStruct((parts * steps, block, LANES), jnp.float32),
            jax.ShapeDtypeStruct(student.shape, jnp.bfloat16),
        ],
        scratch_shapes=[
            pltpu.VMEM((block, keys), jnp.float32),
            pltpu.VMEM((block, keys), jnp.float32),
            pltpu.VMEM((block, keys), jnp.bfloat16),
        ] * 2 + [pltpu.VMEM((group, keys), jnp.float32)] * 4 + [
            pltpu.VMEM((s_width, keys), jnp.float32),
            pltpu.VMEM((s_width, keys), jnp.float32),
        ],
        compiler_params=pltpu.CompilerParams(
            dimension_semantics=("arbitrary",), vmem_limit_bytes=60 * 1024 * 1024
        ),
        name="relation",
    )(teacher, student, student.T)
    return kl[:, :, 0].reshape(parts, keys), grad


MESH = pl.DeviceIdType.MESH


def gather_body(
    teacher, hidden, weight, teacher_out, student_out, hidden_out,
    h_full, w_full, total, s_loc, t_stage, h_send, h_recv, w_up, w_down, w_side, w_recv, w_side_recv,
    t_send, t_recv, s_send, s_recv, local_sem,
    *, line, pairs, members, tps,
):
    dp = lax.axis_index("dp")
    tp = lax.axis_index("tp")
    z, x = dp // pairs, dp % pairs
    size = line * pairs
    base = dp // members * members
    spot = dp % members
    token_rows = hidden.shape[0]
    feats = hidden.shape[1]
    depth = weight.shape[0]
    width = weight.shape[1]

    barrier = pltpu.get_barrier_semaphore()
    for k in range(1, size):
        pl.semaphore_signal(barrier, inc=1, device_id={"dp": (dp + k) % size}, device_id_type=MESH)
    for k in range(1, tps):
        pl.semaphore_signal(barrier, inc=1, device_id={"tp": (tp + k) % tps}, device_id_type=MESH)
    pl.semaphore_wait(barrier, size - 1 + tps - 1)

    half = tp // 2
    core = tp % 2
    mate = half * 2 + 1 - core
    across = (1 - half) * 2 + core
    side = z * pairs + 1 - x

    def feat_cols(owner):
        return pl.ds(pl.multiple_of(owner * feats, feats), feats)

    def weight_rows(zo, xo):
        return pl.ds(pl.multiple_of((zo * pairs + xo) * depth, depth), depth)

    def remote(src, dst, send, recv, where):
        return pltpu.make_async_remote_copy(
            src_ref=src, dst_ref=dst, send_sem=send, recv_sem=recv, device_id=where, device_id_type=MESH
        )

    def hidden_copy(n, src, owner, where):
        return remote(src, h_full.at[:, feat_cols(owner)], h_send.at[n], h_recv.at[n], where)

    def weight_copy(src, zo, sems, where):
        return remote(src, w_full.at[weight_rows(zo, x), :], sems.at[zo], w_recv.at[zo], where)

    def weight_aside(src, zo, xo):
        return remote(src, w_full.at[weight_rows(zo, xo), :], w_side.at[zo], w_side_recv.at[zo], {"dp": side})

    def onward(src, zo, up, down):
        if up:
            @pl.when(z < line - 1)
            def _():
                weight_copy(src, zo, w_up, {"dp": dp + pairs}).start()
        if down:
            @pl.when(z > 0)
            def _():
                weight_copy(src, zo, w_down, {"dp": dp - pairs}).start()
        weight_aside(src, zo, x).start()

    hidden_copy(0, hidden, tp, {"tp": across}).start()
    hidden_copy(1, hidden, tp, {"tp": mate}).start()
    onward(weight, z, True, True)
    h_own = pltpu.make_async_copy(hidden, h_full.at[:, feat_cols(tp)], local_sem.at[0])
    h_own.start()
    w_own = pltpu.make_async_copy(weight, w_full.at[weight_rows(z, x), :], local_sem.at[1])
    w_own.start()
    t_cols = teacher.shape[1] // members
    s_cols = width // members

    def part(k, n):
        return pl.ds(pl.multiple_of(k * n, n), n)

    own_rows = part(spot, token_rows)
    t_in = pltpu.make_async_copy(teacher.at[:, part(spot, t_cols)], t_stage, local_sem.at[2])
    t_in.start()

    def step(d, below):
        zo = z - d if below else z + d
        there = zo >= 0 if below else zo < line
        return zo, there

    def arrive(d):
        for below in (True, False):
            zo, there = step(d, below)

            @pl.when(there)
            def _():
                weight_copy(w_full.at[weight_rows(zo, x), :], zo, w_up, {"dp": dp}).wait_recv()
                onward(w_full.at[weight_rows(zo, x), :], zo, below, not below)

    def add(zo, xo, first=False):
        rows = 256 if token_rows % 256 == 0 else token_rows
        cols = 256 if width % 256 == 0 else width
        span = weight_rows(zo, xo)

        def tile(i, carry):
            at = part(i // (width // cols), rows)
            to = part(i % (width // cols), cols)
            term = jnp.dot(h_full[at, span], w_full[span, to], preferred_element_type=jnp.float32)
            total[at, to] = term if first else total[at, to] + term
            return carry

        lax.fori_loop(0, (token_rows // rows) * (width // cols), tile, 0)

    def add_mine(d):
        for below in (True, False):
            zo, there = step(d, below)

            @pl.when(there)
            def _():
                add(zo, x)

    def add_side(d):
        for below in (True, False) if d else (True,):
            zo, there = step(d, below)

            @pl.when(there)
            def _():
                weight_aside(w_full.at[weight_rows(zo, 1 - x), :], zo, 1 - x).wait_recv()
                add(zo, 1 - x)

    arrive(1)
    hidden_copy(0, hidden, across, {"tp": across}).wait_recv()
    hidden_copy(2, h_full.at[:, feat_cols(across)], across, {"tp": mate}).start()
    hidden_copy(1, hidden, mate, {"tp": mate}).wait_recv()
    h_own.wait()
    w_own.wait()
    far = (1 - half) * 2 + 1 - core
    hidden_copy(2, hidden, far, {"tp": mate}).wait_recv()
    h_out = pltpu.make_async_copy(h_full, hidden_out, local_sem.at[0])
    h_out.start()
    add(z, x, True)
    add_side(0)
    add_mine(1)
    for d in range(2, line):
        arrive(d)
        if d == line - 1:
            for k in range(1, members):
                to = (spot + k) % members
                remote(
                    teacher.at[:, part(to, t_cols)], teacher_out.at[own_rows, :], t_send.at[k], t_recv.at[k], {"dp": base + to}
                ).start()
        add_side(d - 1)
        add_mine(d)
    add_side(line - 1)

    s_loc[...] = total[...].astype(jnp.bfloat16)
    for k in range(1, members):
        to = (spot + k) % members
        remote(
            s_loc.at[:, part(to, s_cols)], student_out.at[own_rows, :], s_send.at[k], s_recv.at[k], {"dp": base + to}
        ).start()
    t_in.wait()
    t_out = pltpu.make_async_copy(t_stage, teacher_out.at[own_rows, :], local_sem.at[2])
    t_out.start()
    s_own = pltpu.make_async_copy(s_loc.at[:, part(spot, s_cols)], student_out.at[own_rows, :], local_sem.at[1])
    s_own.start()

    hidden_copy(0, hidden, tp, {"tp": across}).wait_send()
    hidden_copy(1, hidden, tp, {"tp": mate}).wait_send()
    hidden_copy(2, hidden, across, {"tp": mate}).wait_send()
    for d in range(line):
        for below in (True, False) if d else (True,):
            zo, there = step(d, below)

            @pl.when(jnp.logical_and(there, z < line - 1) if below else False)
            def _():
                weight_copy(weight, zo, w_up, {"dp": dp}).wait_send()

            @pl.when(jnp.logical_and(there, z > 0) if not below or d == 0 else False)
            def _():
                weight_copy(weight, zo, w_down, {"dp": dp}).wait_send()

            @pl.when(there)
            def _():
                weight_aside(weight, zo, x).wait_send()
    for k in range(1, members):
        source = (spot + members - k) % members
        from_rows = part(source, token_rows)
        t_copy = remote(
            teacher.at[:, part(spot, t_cols)], teacher_out.at[from_rows, :], t_send.at[k], t_recv.at[k], {"dp": base + source}
        )
        s_copy = remote(
            s_loc.at[:, part(spot, s_cols)], student_out.at[from_rows, :], s_send.at[k], s_recv.at[k], {"dp": base + source}
        )
        t_copy.wait()
        s_copy.wait()
    h_out.wait()
    t_out.wait()
    s_own.wait()


def gather_and_project(teacher_query, student_hidden, query_weight):
    tps, size = lax.axis_size("tp"), lax.axis_size("dp")
    members = size // NSEQ
    pairs = 2
    line = size // pairs
    rows, feats = student_hidden.shape
    depth, width = query_weight.shape
    dma = pltpu.SemaphoreType.DMA
    any_space = pl.BlockSpec(memory_space=pl.ANY)
    return pl.pallas_call(
        functools.partial(gather_body, line=line, pairs=pairs, members=members, tps=tps),
        in_specs=[any_space] * 3,
        out_specs=[any_space] * 3,
        out_shape=[
            jax.ShapeDtypeStruct((members * rows, teacher_query.shape[1] // members), jnp.bfloat16),
            jax.ShapeDtypeStruct((members * rows, width // members), jnp.bfloat16),
            jax.ShapeDtypeStruct((rows, tps * feats), jnp.bfloat16),
        ],
        scratch_shapes=[
            pltpu.VMEM((rows, tps * feats), jnp.bfloat16),
            pltpu.VMEM((size * depth, width), jnp.bfloat16),
            pltpu.VMEM((rows, width), jnp.float32),
            pltpu.VMEM((rows, width), jnp.bfloat16),
            pltpu.VMEM((rows, teacher_query.shape[1] // members), jnp.bfloat16),
            dma((3,)), dma((3,)), dma((line,)), dma((line,)), dma((line,)), dma((line,)), dma((line,)),
            dma((members,)), dma((members,)), dma((members,)), dma((members,)), dma((3,)),
        ],
        compiler_params=pltpu.CompilerParams(
            collective_id=0, has_side_effects=True, vmem_limit_bytes=60 * 1024 * 1024
        ),
        name="gather_and_project",
    )(teacher_query, student_hidden, query_weight)


def heads_of_one_sequence(teacher_query, student_hidden, query_weight):
    members = lax.axis_size("dp") // NSEQ
    mine = RHEADS // lax.axis_size("tp") // members
    groups = [[s * members + k for k in range(members)] for s in range(NSEQ)]
    teacher_all, student_all, hidden_full = gather_and_project(teacher_query, student_hidden, query_weight)
    rows_of = [0.0] * NSEQ
    kl, grad = relation(teacher_all, student_all, mine)
    for m in range(mine):
        for s in range(NSEQ):
            pairs = [(s * members + k, k * mine + m) for k in range(members)]
            rows_of[s] = rows_of[s] + lax.ppermute(kl[m], "dp", pairs)
    grad_rows = lax.all_to_all(
        grad, "dp", split_axis=0, concat_axis=1, axis_index_groups=groups, tiled=True
    )
    partial = lax.dot_general(
        hidden_full, grad_rows, (((0,), (0,)), ((), ())), preferred_element_type=jnp.float32
    )
    size = lax.axis_size("dp")
    pieces = partial.reshape(size, partial.shape[0] // size, partial.shape[1]).astype(jnp.bfloat16)
    landed = lax.all_to_all(pieces, "dp", split_axis=0, concat_axis=0, tiled=True)
    return jnp.concatenate(rows_of).reshape(1, NSEQ * SEQ), jnp.sum(landed.astype(jnp.float32), axis=0)


def local(teacher_query, student_hidden, query_weight):
    heads_here = RHEADS // lax.axis_size("tp")
    copies = lax.axis_size("dp") // heads_here
    if lax.axis_size("dp") % NSEQ == 0 and heads_here % (lax.axis_size("dp") // NSEQ) == 0:
        return heads_of_one_sequence(teacher_query, student_hidden, query_weight)
    rows = teacher_query.shape[0]
    teacher_width = teacher_query.shape[1] // heads_here
    hidden_full = lax.all_gather(student_hidden, "tp", axis=1, tiled=True)
    teacher_send = spread_heads(teacher_query, heads_here, copies)
    projected = jnp.dot(
        hidden_full,
        lax.all_gather(query_weight, "dp", axis=0, tiled=True),
        preferred_element_type=jnp.float32,
    )
    student_query = projected.astype(jnp.bfloat16)
    student_width = student_query.shape[1] // heads_here
    student_send = spread_heads(student_query, heads_here, copies)
    teacher_all, student_all = (
        lax.all_to_all(teacher_send, "dp", split_axis=1, concat_axis=0, tiled=True),
        lax.all_to_all(student_send, "dp", split_axis=1, concat_axis=0, tiled=True),
    )
    total_rows = teacher_all.shape[0]
    teacher_all = teacher_all.reshape(total_rows, teacher_width)
    student_all = student_all.reshape(total_rows, student_width)
    teacher_scale = teacher_width ** (-0.5)
    student_scale = student_width ** (-0.5)
    query_rows = SEQ // copies
    first_row = lax.axis_index("dp") % copies * query_rows
    block = min(512, query_rows)
    blocks_each = query_rows // block

    def relation_step(step, carry):
        kl_store, grad_store = carry
        sequence = step // blocks_each
        offset = step % blocks_each * block
        base = sequence * SEQ
        start = base + first_row + offset
        teacher_keys = lax.dynamic_slice_in_dim(teacher_all, base, SEQ, 0)
        student_keys = lax.dynamic_slice_in_dim(student_all, base, SEQ, 0)
        teacher_rows = lax.dynamic_slice_in_dim(teacher_all, start, block, 0)
        student_rows = lax.dynamic_slice_in_dim(student_all, start, block, 0)
        teacher_scores = (
            lax.dot_general(
                teacher_rows,
                teacher_keys,
                (((1,), (1,)), ((), ())),
                preferred_element_type=jnp.float32,
            )
            * teacher_scale
        )
        student_scores = (
            lax.dot_general(
                student_rows,
                student_keys,
                (((1,), (1,)), ((), ())),
                preferred_element_type=jnp.float32,
            )
            * student_scale
        )
        teacher_log = jax.nn.log_softmax(teacher_scores, axis=-1)
        student_log = jax.nn.log_softmax(student_scores, axis=-1)
        teacher_prob = jnp.exp(teacher_log)
        divergence = jnp.sum(teacher_prob * (teacher_log - student_log), axis=-1)
        score_grad = (jnp.exp(student_log) - teacher_prob).astype(jnp.bfloat16)
        key_part = (
            lax.dot_general(
                score_grad,
                student_rows,
                (((0,), (0,)), ((), ())),
                preferred_element_type=jnp.float32,
            )
            * student_scale
        )
        row_part = (
            jnp.dot(score_grad, student_keys, preferred_element_type=jnp.float32) * student_scale
        )
        seq_grad = lax.dynamic_slice_in_dim(grad_store, base, SEQ, 0)
        grad_store = lax.dynamic_update_slice_in_dim(grad_store, seq_grad + key_part, base, 0)
        current = lax.dynamic_slice_in_dim(grad_store, start, block, 0)
        grad_store = lax.dynamic_update_slice_in_dim(grad_store, current + row_part, start, 0)
        kl_store = lax.dynamic_update_slice_in_dim(
            kl_store, divergence, sequence * query_rows + offset, 0
        )
        return (kl_store, grad_store)

    kl_init = jnp.zeros((NSEQ * query_rows,), jnp.float32)
    grad_init = jnp.zeros((total_rows, student_width), jnp.float32)
    kl_store, grad_store = lax.fori_loop(0, NSEQ * blocks_each, relation_step, (kl_init, grad_init))
    returned = lax.all_to_all(
        grad_store.reshape(heads_here * copies, rows, student_width),
        "dp",
        split_axis=0,
        concat_axis=2,
        tiled=True,
    )
    summed = jnp.sum(returned.reshape(rows, heads_here, copies, student_width), axis=2)
    query_grad = summed.reshape(rows, heads_here * student_width).astype(jnp.bfloat16)
    weight_grad = lax.psum_scatter(
        lax.dot_general(
            hidden_full, query_grad, (((0,), (0,)), ((), ())), preferred_element_type=jnp.float32
        ),
        "dp",
        scatter_dimension=0,
        tiled=True,
    )
    return (kl_store.reshape(1, NSEQ * query_rows), weight_grad)


def solution(mesh):
    placed = (P("dp", "tp"), P("dp", "tp"), P("dp", "tp"))
    return jax.shard_map(
        local,
        mesh=mesh,
        in_specs=placed,
        out_specs=(P(("tp", "dp"), None), P("dp", "tp")),
        check_vma=False,
    )
```

```python
import functools
import math

import jax
import jax.numpy as jnp
from jax import lax
from jax.experimental import pallas as pl
from jax.experimental.pallas import tpu as pltpu
from jax.sharding import PartitionSpec as P

RHEADS = 32
NSEQ = 2
SEQ = 4096


def spread_heads(queries, heads, copies):
    rows = queries.shape[0]
    width = queries.shape[1] // heads
    shaped = queries.reshape(rows, heads, 1, width)
    return jnp.broadcast_to(shaped, (rows, heads, copies, width)).reshape(
        rows, heads * copies, width
    )

LOG2E = 1.0 / math.log(2.0)
LN2 = math.log(2.0)
LANES = 128


NT = (((1,), (1,)), ((), ()))


def stage(t_keys, s_keys, s_turned, kl_out, t_new, s_new, t_old, s_old, g_new, g_old, exps, row_acc, key_acc,
          *, score_row, grad_row, group, t_scale, s_scale):
    block, keys = t_new.shape
    groups = block // group
    pieces = groups // 2
    chunk = keys // pieces
    tiles = keys // LANES
    ct = t_scale * LOG2E
    cs = s_scale * LOG2E
    rows = pl.ds(pl.multiple_of(score_row, block), block)
    old_rows = pl.ds(pl.multiple_of(grad_row, block), block)

    def rows_at(i):
        return pl.ds(pl.multiple_of(i * group, group), group)

    def tops(i):
        at = rows_at(i)
        t_max = t_old[at, 0:LANES]
        s_max = s_old[at, 0:LANES]
        for k in range(1, tiles):
            c = slice(k * LANES, (k + 1) * LANES)
            t_max = jnp.maximum(t_max, t_old[at, c])
            s_max = jnp.maximum(s_max, s_old[at, c])
        return (
            jnp.broadcast_to(jnp.max(t_max, axis=1, keepdims=True), (group, LANES)),
            jnp.broadcast_to(jnp.max(s_max, axis=1, keepdims=True), (group, LANES)),
        )

    def sums(i, t_max, s_max, t_e, s_e):
        at = rows_at(i)
        t_sum = jnp.zeros((group, LANES), jnp.float32)
        s_sum = jnp.zeros((group, LANES), jnp.float32)
        gap = jnp.zeros((group, LANES), jnp.float32)
        for k in range(tiles):
            c = slice(k * LANES, (k + 1) * LANES)
            u = (t_old[at, c] - t_max) * ct
            v = (s_old[at, c] - s_max) * cs
            t_exp = jnp.exp2(u)
            s_exp = jnp.exp2(v)
            t_e[:, c] = t_exp
            s_e[:, c] = s_exp
            t_sum = t_sum + t_exp
            s_sum = s_sum + s_exp
            gap = gap + t_exp * (u - v)
        t_sum = jnp.sum(t_sum, axis=1, keepdims=True)
        s_sum = jnp.sum(s_sum, axis=1, keepdims=True)
        gap = jnp.sum(gap, axis=1, keepdims=True)
        kl = gap * LN2 / t_sum - jnp.log(t_sum) + jnp.log(s_sum)
        kl_out[0, at, :] = jnp.broadcast_to(kl, (group, LANES))
        return jnp.broadcast_to(1.0 / t_sum, (group, LANES)), jnp.broadcast_to(1.0 / s_sum, (group, LANES))

    def score_grads(i, t_inv, s_inv, t_e, s_e):
        at = rows_at(i)
        for k in range(tiles):
            c = slice(k * LANES, (k + 1) * LANES)
            g_new[at, c] = (s_e[:, c] * s_inv - t_e[:, c] * t_inv).astype(jnp.bfloat16)

    def matmuls(i):
        half = chunk // 2
        for h in range(2):
            cols = pl.ds(pl.multiple_of(i * chunk + h * half, half), half)
            t_new[:, cols] = lax.dot_general(t_keys[rows, :], t_keys[cols, :], NT, preferred_element_type=jnp.float32)
            s_new[:, cols] = lax.dot_general(s_keys[rows, :], s_keys[cols, :], NT, preferred_element_type=jnp.float32)
            key_acc[:, cols] += jnp.dot(s_turned[:, old_rows], g_old[:, cols], preferred_element_type=jnp.float32)
        cols = pl.ds(pl.multiple_of(i * chunk, chunk), chunk)
        row_acc[:, old_rows] += lax.dot_general(
            s_turned[:, cols], g_old[:, cols], NT, preferred_element_type=jnp.float32
        )

    t_even, s_even, t_odd, s_odd = exps

    def work(i, carry):
        even_max, odd_inv = carry
        matmuls(i)
        odd_max = tops(2 * i + 1)
        score_grads(jnp.maximum(2 * i - 1, 0), *odd_inv, t_odd, s_odd)
        even_inv = sums(2 * i, *even_max, t_even, s_even)
        next_max = tops(jnp.minimum(2 * i + 2, groups - 1))
        score_grads(2 * i, *even_inv, t_even, s_even)
        odd_inv = sums(2 * i + 1, *odd_max, t_odd, s_odd)
        return next_max, odd_inv

    zero = jnp.zeros((group, LANES), jnp.float32)
    _, odd_inv = lax.fori_loop(0, pieces, work, (tops(0), (zero, zero)))
    score_grads(groups - 1, *odd_inv, t_odd, s_odd)


def relation_body(t_keys, s_keys, s_turned, kl_out, grad_out,
                  t_a, s_a, g_a, t_b, s_b, g_b, t_even, s_even, t_odd, s_odd, row_acc, key_acc, *, steps, group, t_scale, s_scale):
    step = pl.program_id(0)
    block = t_a.shape[0]
    keys = t_a.shape[1]
    last = pl.num_programs(0) - 3
    score_row = jnp.minimum(step, last) % steps * block
    grad_row = jnp.maximum(step - 2, 0) % steps * block

    @pl.when(jnp.logical_or(step < 2, (step - 2) % steps == 0))
    def _():
        row_acc[...] = jnp.zeros_like(row_acc)
        key_acc[...] = jnp.zeros_like(key_acc)

    for parity, (t_new, s_new, g_new, t_old, s_old, g_old) in enumerate(
        ((t_a, s_a, g_a, t_b, s_b, g_b), (t_b, s_b, g_b, t_a, s_a, g_a))
    ):
        @pl.when(step % 2 == parity)
        def _():
            stage(t_keys, s_keys, s_turned, kl_out, t_new, s_new, t_old, s_old, g_new, g_old,
                  (t_even, s_even, t_odd, s_odd), row_acc, key_acc,
                  score_row=score_row, grad_row=grad_row, group=group, t_scale=t_scale, s_scale=s_scale)

    @pl.when(jnp.logical_and(step >= 2, (step - 2) % steps == steps - 1))
    def _():
        def finish(c, carry):
            at = pl.ds(pl.multiple_of(c * LANES, LANES), LANES)
            grad_out[at, :] = ((row_acc[:, at] + key_acc[:, at]).T * s_scale).astype(jnp.bfloat16)
            return carry
        lax.fori_loop(0, keys // LANES, finish, 0)


def relation(teacher, student, parts):
    keys = teacher.shape[0]
    t_width = teacher.shape[1] // parts
    s_width = student.shape[1] // parts
    block = min(256, keys)
    group = 32
    steps = keys // block
    last = parts * steps - 1
    score_part = lambda i: jnp.minimum(i, last) // steps
    grad_part = lambda i: jnp.maximum(i - 2, 0) // steps
    kl, grad = pl.pallas_call(
        functools.partial(relation_body, steps=steps, group=group, t_scale=t_width ** (-0.5), s_scale=s_width ** (-0.5)),
        grid=(parts * steps + 2,),
        in_specs=[
            pl.BlockSpec((keys, t_width), lambda i: (0, score_part(i))),
            pl.BlockSpec((keys, s_width), lambda i: (0, score_part(i))),
            pl.BlockSpec((s_width, keys), lambda i: (grad_part(i), 0)),
        ],
        out_specs=[
            pl.BlockSpec((1, block, LANES), lambda i: (jnp.clip(i - 1, 0, last), 0, 0)),
            pl.BlockSpec((keys, s_width), lambda i: (0, grad_part(i))),
        ],
        out_shape=[
            jax.ShapeDtypeStruct((parts * steps, block, LANES), jnp.float32),
            jax.ShapeDtypeStruct(student.shape, jnp.bfloat16),
        ],
        scratch_shapes=[
            pltpu.VMEM((block, keys), jnp.float32),
            pltpu.VMEM((block, keys), jnp.float32),
            pltpu.VMEM((block, keys), jnp.bfloat16),
        ] * 2 + [pltpu.VMEM((group, keys), jnp.float32)] * 4 + [
            pltpu.VMEM((s_width, keys), jnp.float32),
            pltpu.VMEM((s_width, keys), jnp.float32),
        ],
        compiler_params=pltpu.CompilerParams(
            dimension_semantics=("arbitrary",), vmem_limit_bytes=60 * 1024 * 1024
        ),
        name="relation",
    )(teacher, student, student.T)
    return kl[:, :, 0].reshape(parts, keys), grad


MESH = pl.DeviceIdType.MESH


def gather_body(
    teacher, hidden, weight, teacher_out, student_out, hidden_out,
    h_full, w_full, total, s_loc, t_stage, h_send, h_recv, w_up, w_down, w_side, w_recv, w_side_recv,
    t_send, t_recv, s_send, s_recv, local_sem,
    *, line, pairs, members, tps,
):
    dp = lax.axis_index("dp")
    tp = lax.axis_index("tp")
    z, x = dp // pairs, dp % pairs
    size = line * pairs
    base = dp // members * members
    spot = dp % members
    token_rows = hidden.shape[0]
    feats = hidden.shape[1]
    depth = weight.shape[0]
    width = weight.shape[1]

    barrier = pltpu.get_barrier_semaphore()
    for k in range(1, size):
        pl.semaphore_signal(barrier, inc=1, device_id={"dp": (dp + k) % size}, device_id_type=MESH)
    for k in range(1, tps):
        pl.semaphore_signal(barrier, inc=1, device_id={"tp": (tp + k) % tps}, device_id_type=MESH)
    pl.semaphore_wait(barrier, size - 1 + tps - 1)

    half = tp // 2
    core = tp % 2
    mate = half * 2 + 1 - core
    across = (1 - half) * 2 + core
    side = z * pairs + 1 - x

    def feat_cols(owner):
        return pl.ds(pl.multiple_of(owner * feats, feats), feats)

    def weight_rows(zo, xo):
        return pl.ds(pl.multiple_of((zo * pairs + xo) * depth, depth), depth)

    def remote(src, dst, send, recv, where):
        return pltpu.make_async_remote_copy(
            src_ref=src, dst_ref=dst, send_sem=send, recv_sem=recv, device_id=where, device_id_type=MESH
        )

    def hidden_copy(n, src, owner, where):
        return remote(src, h_full.at[:, feat_cols(owner)], h_send.at[n], h_recv.at[n], where)

    def weight_copy(src, zo, sems, where):
        return remote(src, w_full.at[weight_rows(zo, x), :], sems.at[zo], w_recv.at[zo], where)

    def weight_aside(src, zo, xo):
        return remote(src, w_full.at[weight_rows(zo, xo), :], w_side.at[zo], w_side_recv.at[zo], {"dp": side})

    def onward(src, zo, up, down):
        if up:
            @pl.when(z < line - 1)
            def _():
                weight_copy(src, zo, w_up, {"dp": dp + pairs}).start()
        if down:
            @pl.when(z > 0)
            def _():
                weight_copy(src, zo, w_down, {"dp": dp - pairs}).start()
        weight_aside(src, zo, x).start()

    hidden_copy(0, hidden, tp, {"tp": across}).start()
    hidden_copy(1, hidden, tp, {"tp": mate}).start()
    onward(weight, z, True, True)
    h_own = pltpu.make_async_copy(hidden, h_full.at[:, feat_cols(tp)], local_sem.at[0])
    h_own.start()
    w_own = pltpu.make_async_copy(weight, w_full.at[weight_rows(z, x), :], local_sem.at[1])
    w_own.start()
    t_cols = teacher.shape[1] // members
    s_cols = width // members

    def part(k, n):
        return pl.ds(pl.multiple_of(k * n, n), n)

    own_rows = part(spot, token_rows)
    t_in = pltpu.make_async_copy(teacher.at[:, part(spot, t_cols)], t_stage, local_sem.at[2])
    t_in.start()

    def step(d, below):
        zo = z - d if below else z + d
        there = zo >= 0 if below else zo < line
        return zo, there

    def arrive(d):
        for below in (True, False):
            zo, there = step(d, below)

            @pl.when(there)
            def _():
                weight_copy(w_full.at[weight_rows(zo, x), :], zo, w_up, {"dp": dp}).wait_recv()
                onward(w_full.at[weight_rows(zo, x), :], zo, below, not below)

    def add(zo, xo, first=False):
        rows = 256 if token_rows % 256 == 0 else token_rows
        cols = 256 if width % 256 == 0 else width
        span = weight_rows(zo, xo)

        def tile(i, carry):
            at = part(i // (width // cols), rows)
            to = part(i % (width // cols), cols)
            term = jnp.dot(h_full[at, span], w_full[span, to], preferred_element_type=jnp.float32)
            total[at, to] = term if first else total[at, to] + term
            return carry

        lax.fori_loop(0, (token_rows // rows) * (width // cols), tile, 0)

    def add_mine(d):
        for below in (True, False):
            zo, there = step(d, below)

            @pl.when(there)
            def _():
                add(zo, x)

    def add_side(d):
        for below in (True, False) if d else (True,):
            zo, there = step(d, below)

            @pl.when(there)
            def _():
                weight_aside(w_full.at[weight_rows(zo, 1 - x), :], zo, 1 - x).wait_recv()
                add(zo, 1 - x)

    arrive(1)
    hidden_copy(0, hidden, across, {"tp": across}).wait_recv()
    hidden_copy(2, h_full.at[:, feat_cols(across)], across, {"tp": mate}).start()
    hidden_copy(1, hidden, mate, {"tp": mate}).wait_recv()
    h_own.wait()
    w_own.wait()
    far = (1 - half) * 2 + 1 - core
    hidden_copy(2, hidden, far, {"tp": mate}).wait_recv()
    h_out = pltpu.make_async_copy(h_full, hidden_out, local_sem.at[0])
    h_out.start()
    add(z, x, True)
    add_side(0)
    add_mine(1)
    for d in range(2, line):
        arrive(d)
        if d == line - 1:
            for k in range(1, members):
                to = (spot + k) % members
                remote(
                    teacher.at[:, part(to, t_cols)], teacher_out.at[own_rows, :], t_send.at[k], t_recv.at[k], {"dp": base + to}
                ).start()
        add_side(d - 1)
        add_mine(d)
    add_side(line - 1)

    s_loc[...] = total[...].astype(jnp.bfloat16)
    for k in range(1, members):
        to = (spot + k) % members
        remote(
            s_loc.at[:, part(to, s_cols)], student_out.at[own_rows, :], s_send.at[k], s_recv.at[k], {"dp": base + to}
        ).start()
    t_in.wait()
    t_out = pltpu.make_async_copy(t_stage, teacher_out.at[own_rows, :], local_sem.at[2])
    t_out.start()
    s_own = pltpu.make_async_copy(s_loc.at[:, part(spot, s_cols)], student_out.at[own_rows, :], local_sem.at[1])
    s_own.start()

    hidden_copy(0, hidden, tp, {"tp": across}).wait_send()
    hidden_copy(1, hidden, tp, {"tp": mate}).wait_send()
    hidden_copy(2, hidden, across, {"tp": mate}).wait_send()
    for d in range(line):
        for below in (True, False) if d else (True,):
            zo, there = step(d, below)

            @pl.when(jnp.logical_and(there, z < line - 1) if below else False)
            def _():
                weight_copy(weight, zo, w_up, {"dp": dp}).wait_send()

            @pl.when(jnp.logical_and(there, z > 0) if not below or d == 0 else False)
            def _():
                weight_copy(weight, zo, w_down, {"dp": dp}).wait_send()

            @pl.when(there)
            def _():
                weight_aside(weight, zo, x).wait_send()
    for k in range(1, members):
        source = (spot + members - k) % members
        from_rows = part(source, token_rows)
        t_copy = remote(
            teacher.at[:, part(spot, t_cols)], teacher_out.at[from_rows, :], t_send.at[k], t_recv.at[k], {"dp": base + source}
        )
        s_copy = remote(
            s_loc.at[:, part(spot, s_cols)], student_out.at[from_rows, :], s_send.at[k], s_recv.at[k], {"dp": base + source}
        )
        t_copy.wait()
        s_copy.wait()
    h_out.wait()
    t_out.wait()
    s_own.wait()


def gather_and_project(teacher_query, student_hidden, query_weight):
    tps, size = lax.axis_size("tp"), lax.axis_size("dp")
    members = size // NSEQ
    pairs = 2
    line = size // pairs
    rows, feats = student_hidden.shape
    depth, width = query_weight.shape
    dma = pltpu.SemaphoreType.DMA
    any_space = pl.BlockSpec(memory_space=pl.ANY)
    return pl.pallas_call(
        functools.partial(gather_body, line=line, pairs=pairs, members=members, tps=tps),
        in_specs=[any_space] * 3,
        out_specs=[any_space] * 3,
        out_shape=[
            jax.ShapeDtypeStruct((members * rows, teacher_query.shape[1] // members), jnp.bfloat16),
            jax.ShapeDtypeStruct((members * rows, width // members), jnp.bfloat16),
            jax.ShapeDtypeStruct((rows, tps * feats), jnp.bfloat16),
        ],
        scratch_shapes=[
            pltpu.VMEM((rows, tps * feats), jnp.bfloat16),
            pltpu.VMEM((size * depth, width), jnp.bfloat16),
            pltpu.VMEM((rows, width), jnp.float32),
            pltpu.VMEM((rows, width), jnp.bfloat16),
            pltpu.VMEM((rows, teacher_query.shape[1] // members), jnp.bfloat16),
            dma((3,)), dma((3,)), dma((line,)), dma((line,)), dma((line,)), dma((line,)), dma((line,)),
            dma((members,)), dma((members,)), dma((members,)), dma((members,)), dma((3,)),
        ],
        compiler_params=pltpu.CompilerParams(
            collective_id=0, has_side_effects=True, vmem_limit_bytes=60 * 1024 * 1024
        ),
        name="gather_and_project",
    )(teacher_query, student_hidden, query_weight)


def reduce_body(
    hidden, grad, out, h_all, g_all, own, x_out, x_in, z_out, z_in,
    g_send, g_recv, x_send, x_recv, z_send, z_recv, local_sem,
    *, line, pairs, members,
):
    dp = lax.axis_index("dp")
    z, x = dp // pairs, dp % pairs
    size = line * pairs
    base = dp // members * members
    spot = dp % members
    token_rows = h_all.shape[0]
    depth = out.shape[0]
    g_cols = grad.shape[1]
    tall = 256 if depth % 256 == 0 else depth

    barrier = pltpu.get_barrier_semaphore()
    for k in range(1, size):
        pl.semaphore_signal(barrier, inc=1, device_id={"dp": (dp + k) % size}, device_id_type=MESH)
    h_in = pltpu.make_async_copy(hidden, h_all, local_sem.at[0])
    h_in.start()
    pl.semaphore_wait(barrier, size - 1)

    def part(k, n):
        return pl.ds(pl.multiple_of(k * n, n), n)

    def remote(src, dst, send, recv, to):
        return pltpu.make_async_remote_copy(
            src_ref=src, dst_ref=dst, send_sem=send, recv_sem=recv, device_id={"dp": to}, device_id_type=MESH
        )

    def grad_copy(k, to):
        return remote(
            grad.at[part(to % members, token_rows), :], g_all.at[:, part(spot, g_cols)], g_send.at[k], g_recv.at[k], to
        )

    for k in range(1, members):
        grad_copy(k, base + (spot + k) % members).start()
    g_own = pltpu.make_async_copy(
        grad.at[part(spot, token_rows), :], g_all.at[:, part(spot, g_cols)], local_sem.at[1]
    )
    g_own.start()
    h_in.wait()
    g_own.wait()
    for k in range(1, members):
        grad_copy(k, base + (spot + members - k) % members).wait_recv()

    shifts = [line // 2] + [s for s in range(line - 1, 0, -1) if s != line // 2] + [0]

    def multiply(zo, xo, into):
        def tile(i, carry):
            at = pl.ds(pl.multiple_of((zo * pairs + xo) * depth + i * tall, tall), tall)
            term = lax.dot_general(
                h_all[:, at], g_all[...], (((0,), (0,)), ((), ())), preferred_element_type=jnp.float32
            )
            into[part(i, tall), :] = term.astype(into.dtype)
            return carry

        lax.fori_loop(0, depth // tall, tile, 0)

    def aside(n):
        return remote(x_out.at[n], x_in.at[n], x_send.at[n], x_recv.at[n], z * pairs + 1 - x)

    def along(s, zo):
        return remote(z_out.at[s], z_in.at[s], z_send.at[s], z_recv.at[s], zo * pairs + x)

    for n, s in enumerate(shifts):
        multiply((z + s) % line, 1 - x, x_out.at[n])
        aside(n).start()
    for n, s in enumerate(shifts):
        multiply((z + s) % line, x, own.at[n])
    for n, s in enumerate(shifts):
        aside(n).wait_recv()
        if s:
            z_out[s] = (own[n] + x_in[n].astype(jnp.float32)).astype(jnp.bfloat16)
            along(s, (z + s) % line).start()
        else:
            own[n] = own[n] + x_in[n].astype(jnp.float32)
    for s in shifts[:-1]:
        along(s, (z + s) % line).wait_recv()
    total = own[line - 1]
    for s in shifts[:-1]:
        total = total + z_in[s].astype(jnp.float32)
    out[...] = total

    for k in range(1, members):
        grad_copy(k, base + (spot + k) % members).wait_send()
    for n, s in enumerate(shifts):
        aside(n).wait_send()
        if s:
            along(s, (z + s) % line).wait_send()


def reduce_weight(hidden_full, grad):
    size = lax.axis_size("dp")
    members = size // NSEQ
    pairs = 2
    line = size // pairs
    rows, feats = hidden_full.shape
    width = grad.shape[1] * members
    depth = feats // size
    dma = pltpu.SemaphoreType.DMA
    any_space = pl.BlockSpec(memory_space=pl.ANY)
    return pl.pallas_call(
        functools.partial(reduce_body, line=line, pairs=pairs, members=members),
        in_specs=[any_space] * 2,
        out_specs=pl.BlockSpec(memory_space=pltpu.VMEM),
        out_shape=jax.ShapeDtypeStruct((depth, width), jnp.float32),
        scratch_shapes=[
            pltpu.VMEM((rows, feats), jnp.bfloat16),
            pltpu.VMEM((rows, width), jnp.bfloat16),
            pltpu.VMEM((line, depth, width), jnp.float32),
            pltpu.VMEM((line, depth, width), jnp.bfloat16),
            pltpu.VMEM((line, depth, width), jnp.bfloat16),
            pltpu.VMEM((line, depth, width), jnp.bfloat16),
            pltpu.VMEM((line, depth, width), jnp.bfloat16),
            dma((members,)), dma((members,)), dma((line,)), dma((line,)), dma((line,)), dma((line,)), dma((2,)),
        ],
        compiler_params=pltpu.CompilerParams(
            collective_id=1, has_side_effects=True, vmem_limit_bytes=60 * 1024 * 1024
        ),
        name="reduce_weight",
    )(hidden_full, grad)


def heads_of_one_sequence(teacher_query, student_hidden, query_weight):
    members = lax.axis_size("dp") // NSEQ
    mine = RHEADS // lax.axis_size("tp") // members
    groups = [[s * members + k for k in range(members)] for s in range(NSEQ)]
    teacher_all, student_all, hidden_full = gather_and_project(teacher_query, student_hidden, query_weight)
    rows_of = [0.0] * NSEQ
    kl, grad = relation(teacher_all, student_all, mine)
    for m in range(mine):
        for s in range(NSEQ):
            pairs = [(s * members + k, k * mine + m) for k in range(members)]
            rows_of[s] = rows_of[s] + lax.ppermute(kl[m], "dp", pairs)
    weight_grad = reduce_weight(hidden_full, grad)
    return jnp.concatenate(rows_of).reshape(1, NSEQ * SEQ), weight_grad


def local(teacher_query, student_hidden, query_weight):
    heads_here = RHEADS // lax.axis_size("tp")
    copies = lax.axis_size("dp") // heads_here
    if lax.axis_size("dp") % NSEQ == 0 and heads_here % (lax.axis_size("dp") // NSEQ) == 0:
        return heads_of_one_sequence(teacher_query, student_hidden, query_weight)
    rows = teacher_query.shape[0]
    teacher_width = teacher_query.shape[1] // heads_here
    hidden_full = lax.all_gather(student_hidden, "tp", axis=1, tiled=True)
    teacher_send = spread_heads(teacher_query, heads_here, copies)
    projected = jnp.dot(
        hidden_full,
        lax.all_gather(query_weight, "dp", axis=0, tiled=True),
        preferred_element_type=jnp.float32,
    )
    student_query = projected.astype(jnp.bfloat16)
    student_width = student_query.shape[1] // heads_here
    student_send = spread_heads(student_query, heads_here, copies)
    teacher_all, student_all = (
        lax.all_to_all(teacher_send, "dp", split_axis=1, concat_axis=0, tiled=True),
        lax.all_to_all(student_send, "dp", split_axis=1, concat_axis=0, tiled=True),
    )
    total_rows = teacher_all.shape[0]
    teacher_all = teacher_all.reshape(total_rows, teacher_width)
    student_all = student_all.reshape(total_rows, student_width)
    teacher_scale = teacher_width ** (-0.5)
    student_scale = student_width ** (-0.5)
    query_rows = SEQ // copies
    first_row = lax.axis_index("dp") % copies * query_rows
    block = min(512, query_rows)
    blocks_each = query_rows // block

    def relation_step(step, carry):
        kl_store, grad_store = carry
        sequence = step // blocks_each
        offset = step % blocks_each * block
        base = sequence * SEQ
        start = base + first_row + offset
        teacher_keys = lax.dynamic_slice_in_dim(teacher_all, base, SEQ, 0)
        student_keys = lax.dynamic_slice_in_dim(student_all, base, SEQ, 0)
        teacher_rows = lax.dynamic_slice_in_dim(teacher_all, start, block, 0)
        student_rows = lax.dynamic_slice_in_dim(student_all, start, block, 0)
        teacher_scores = (
            lax.dot_general(
                teacher_rows,
                teacher_keys,
                (((1,), (1,)), ((), ())),
                preferred_element_type=jnp.float32,
            )
            * teacher_scale
        )
        student_scores = (
            lax.dot_general(
                student_rows,
                student_keys,
                (((1,), (1,)), ((), ())),
                preferred_element_type=jnp.float32,
            )
            * student_scale
        )
        teacher_log = jax.nn.log_softmax(teacher_scores, axis=-1)
        student_log = jax.nn.log_softmax(student_scores, axis=-1)
        teacher_prob = jnp.exp(teacher_log)
        divergence = jnp.sum(teacher_prob * (teacher_log - student_log), axis=-1)
        score_grad = (jnp.exp(student_log) - teacher_prob).astype(jnp.bfloat16)
        key_part = (
            lax.dot_general(
                score_grad,
                student_rows,
                (((0,), (0,)), ((), ())),
                preferred_element_type=jnp.float32,
            )
            * student_scale
        )
        row_part = (
            jnp.dot(score_grad, student_keys, preferred_element_type=jnp.float32) * student_scale
        )
        seq_grad = lax.dynamic_slice_in_dim(grad_store, base, SEQ, 0)
        grad_store = lax.dynamic_update_slice_in_dim(grad_store, seq_grad + key_part, base, 0)
        current = lax.dynamic_slice_in_dim(grad_store, start, block, 0)
        grad_store = lax.dynamic_update_slice_in_dim(grad_store, current + row_part, start, 0)
        kl_store = lax.dynamic_update_slice_in_dim(
            kl_store, divergence, sequence * query_rows + offset, 0
        )
        return (kl_store, grad_store)

    kl_init = jnp.zeros((NSEQ * query_rows,), jnp.float32)
    grad_init = jnp.zeros((total_rows, student_width), jnp.float32)
    kl_store, grad_store = lax.fori_loop(0, NSEQ * blocks_each, relation_step, (kl_init, grad_init))
    returned = lax.all_to_all(
        grad_store.reshape(heads_here * copies, rows, student_width),
        "dp",
        split_axis=0,
        concat_axis=2,
        tiled=True,
    )
    summed = jnp.sum(returned.reshape(rows, heads_here, copies, student_width), axis=2)
    query_grad = summed.reshape(rows, heads_here * student_width).astype(jnp.bfloat16)
    weight_grad = lax.psum_scatter(
        lax.dot_general(
            hidden_full, query_grad, (((0,), (0,)), ((), ())), preferred_element_type=jnp.float32
        ),
        "dp",
        scatter_dimension=0,
        tiled=True,
    )
    return (kl_store.reshape(1, NSEQ * query_rows), weight_grad)


def solution(mesh):
    placed = (P("dp", "tp"), P("dp", "tp"), P("dp", "tp"))
    return jax.shard_map(
        local,
        mesh=mesh,
        in_specs=placed,
        out_specs=(P(("tp", "dp"), None), P("dp", "tp")),
        check_vma=False,
    )
```

```python
import functools
import math

import jax
import jax.numpy as jnp
from jax import lax
from jax.experimental import pallas as pl
from jax.experimental.pallas import tpu as pltpu
from jax.sharding import PartitionSpec as P

RHEADS = 32
NSEQ = 2
SEQ = 4096


def spread_heads(queries, heads, copies):
    rows = queries.shape[0]
    width = queries.shape[1] // heads
    shaped = queries.reshape(rows, heads, 1, width)
    return jnp.broadcast_to(shaped, (rows, heads, copies, width)).reshape(
        rows, heads * copies, width
    )

LOG2E = 1.0 / math.log(2.0)
LANES = 128


NT = (((1,), (1,)), ((), ()))


def stage(t_keys, s_keys, s_turned, kl_out, t_new, s_new, t_old, s_old, g_new, g_old, exps, row_acc, key_acc,
          *, score_row, grad_row, group, t_scale, s_scale):
    block, keys = t_new.shape
    groups = block // group
    pieces = groups // 2
    chunk = keys // pieces
    tiles = keys // LANES
    ct = t_scale * LOG2E
    cs = s_scale * LOG2E
    rows = pl.ds(pl.multiple_of(score_row, block), block)
    old_rows = pl.ds(pl.multiple_of(grad_row, block), block)

    def rows_at(i):
        return pl.ds(pl.multiple_of(i * group, group), group)

    def tops(i):
        at = rows_at(i)
        t_max = t_old[at, 0:LANES]
        s_max = s_old[at, 0:LANES]
        for k in range(1, tiles):
            c = slice(k * LANES, (k + 1) * LANES)
            t_max = jnp.maximum(t_max, t_old[at, c])
            s_max = jnp.maximum(s_max, s_old[at, c])
        return (
            jnp.broadcast_to(jnp.max(t_max, axis=1, keepdims=True), (group, LANES)),
            jnp.broadcast_to(jnp.max(s_max, axis=1, keepdims=True), (group, LANES)),
        )

    def sums(i, t_max, s_max, t_e, s_e):
        at = rows_at(i)
        t_sum = jnp.zeros((group, LANES), jnp.float32)
        s_sum = jnp.zeros((group, LANES), jnp.float32)
        gap = jnp.zeros((group, LANES), jnp.float32)
        for k in range(tiles):
            c = slice(k * LANES, (k + 1) * LANES)
            t_gap = t_old[at, c] - t_max
            s_gap = s_old[at, c] - s_max
            t_exp = jnp.exp2(t_gap * ct)
            s_exp = jnp.exp2(s_gap * cs)
            t_e[:, c] = t_exp
            s_e[:, c] = s_exp
            t_sum = t_sum + t_exp
            s_sum = s_sum + s_exp
            gap = gap + t_exp * (t_gap - s_gap * (s_scale / t_scale))
        t_sum = jnp.sum(t_sum, axis=1, keepdims=True)
        s_sum = jnp.sum(s_sum, axis=1, keepdims=True)
        gap = jnp.sum(gap, axis=1, keepdims=True)
        kl = gap * t_scale / t_sum - jnp.log(t_sum) + jnp.log(s_sum)
        kl_out[0, at, :] = jnp.broadcast_to(kl, (group, LANES))
        return jnp.broadcast_to(1.0 / t_sum, (group, LANES)), jnp.broadcast_to(1.0 / s_sum, (group, LANES))

    def score_grads(i, t_inv, s_inv, t_e, s_e):
        at = rows_at(i)
        for k in range(tiles):
            c = slice(k * LANES, (k + 1) * LANES)
            g_new[at, c] = (s_e[:, c] * s_inv - t_e[:, c] * t_inv).astype(jnp.bfloat16)

    def matmuls(i):
        half = chunk // 2
        for h in range(2):
            cols = pl.ds(pl.multiple_of(i * chunk + h * half, half), half)
            t_new[:, cols] = lax.dot_general(t_keys[rows, :], t_keys[cols, :], NT, preferred_element_type=jnp.float32)
            s_new[:, cols] = lax.dot_general(s_keys[rows, :], s_keys[cols, :], NT, preferred_element_type=jnp.float32)
            key_acc[:, cols] += jnp.dot(s_turned[:, old_rows], g_old[:, cols], preferred_element_type=jnp.float32)
        cols = pl.ds(pl.multiple_of(i * chunk, chunk), chunk)
        row_acc[:, old_rows] += lax.dot_general(
            s_turned[:, cols], g_old[:, cols], NT, preferred_element_type=jnp.float32
        )

    t_even, s_even, t_odd, s_odd = exps

    def work(i, carry):
        even_max, odd_inv = carry
        matmuls(i)
        odd_max = tops(2 * i + 1)
        score_grads(jnp.maximum(2 * i - 1, 0), *odd_inv, t_odd, s_odd)
        even_inv = sums(2 * i, *even_max, t_even, s_even)
        next_max = tops(jnp.minimum(2 * i + 2, groups - 1))
        score_grads(2 * i, *even_inv, t_even, s_even)
        odd_inv = sums(2 * i + 1, *odd_max, t_odd, s_odd)
        return next_max, odd_inv

    zero = jnp.zeros((group, LANES), jnp.float32)
    _, odd_inv = lax.fori_loop(0, pieces, work, (tops(0), (zero, zero)))
    score_grads(groups - 1, *odd_inv, t_odd, s_odd)


def relation_body(t_keys, s_keys, s_turned, kl_out, grad_out,
                  t_a, s_a, g_a, t_b, s_b, g_b, t_even, s_even, t_odd, s_odd, row_acc, key_acc, *, steps, group, t_scale, s_scale):
    step = pl.program_id(0)
    block = t_a.shape[0]
    keys = t_a.shape[1]
    last = pl.num_programs(0) - 3
    score_row = jnp.minimum(step, last) % steps * block
    grad_row = jnp.maximum(step - 2, 0) % steps * block

    @pl.when(jnp.logical_or(step < 2, (step - 2) % steps == 0))
    def _():
        row_acc[...] = jnp.zeros_like(row_acc)
        key_acc[...] = jnp.zeros_like(key_acc)

    for parity, (t_new, s_new, g_new, t_old, s_old, g_old) in enumerate(
        ((t_a, s_a, g_a, t_b, s_b, g_b), (t_b, s_b, g_b, t_a, s_a, g_a))
    ):
        @pl.when(step % 2 == parity)
        def _():
            stage(t_keys, s_keys, s_turned, kl_out, t_new, s_new, t_old, s_old, g_new, g_old,
                  (t_even, s_even, t_odd, s_odd), row_acc, key_acc,
                  score_row=score_row, grad_row=grad_row, group=group, t_scale=t_scale, s_scale=s_scale)

    @pl.when(jnp.logical_and(step >= 2, (step - 2) % steps == steps - 1))
    def _():
        def finish(c, carry):
            at = pl.ds(pl.multiple_of(c * LANES, LANES), LANES)
            grad_out[at, :] = ((row_acc[:, at] + key_acc[:, at]).T * s_scale).astype(jnp.bfloat16)
            return carry
        lax.fori_loop(0, keys // LANES, finish, 0)


def relation(teacher, student, parts):
    keys = teacher.shape[0]
    t_width = teacher.shape[1] // parts
    s_width = student.shape[1] // parts
    block = min(256, keys)
    group = 32
    steps = keys // block
    last = parts * steps - 1
    score_part = lambda i: jnp.minimum(i, last) // steps
    grad_part = lambda i: jnp.maximum(i - 2, 0) // steps
    kl, grad = pl.pallas_call(
        functools.partial(relation_body, steps=steps, group=group, t_scale=t_width ** (-0.5), s_scale=s_width ** (-0.5)),
        grid=(parts * steps + 2,),
        in_specs=[
            pl.BlockSpec((keys, t_width), lambda i: (0, score_part(i))),
            pl.BlockSpec((keys, s_width), lambda i: (0, score_part(i))),
            pl.BlockSpec((s_width, keys), lambda i: (grad_part(i), 0)),
        ],
        out_specs=[
            pl.BlockSpec((1, block, LANES), lambda i: (jnp.clip(i - 1, 0, last), 0, 0)),
            pl.BlockSpec((keys, s_width), lambda i: (0, grad_part(i))),
        ],
        out_shape=[
            jax.ShapeDtypeStruct((parts * steps, block, LANES), jnp.float32),
            jax.ShapeDtypeStruct(student.shape, jnp.bfloat16),
        ],
        scratch_shapes=[
            pltpu.VMEM((block, keys), jnp.float32),
            pltpu.VMEM((block, keys), jnp.float32),
            pltpu.VMEM((block, keys), jnp.bfloat16),
        ] * 2 + [pltpu.VMEM((group, keys), jnp.float32)] * 4 + [
            pltpu.VMEM((s_width, keys), jnp.float32),
            pltpu.VMEM((s_width, keys), jnp.float32),
        ],
        compiler_params=pltpu.CompilerParams(
            dimension_semantics=("arbitrary",), vmem_limit_bytes=60 * 1024 * 1024
        ),
        name="relation",
    )(teacher, student, student.T)
    return kl[:, :, 0].reshape(parts, keys), grad


MESH = pl.DeviceIdType.MESH


def gather_body(
    teacher, hidden, weight, teacher_out, student_out, hidden_out,
    h_full, w_full, total, s_loc, t_stage, h_send, h_recv, w_up, w_down, w_side, w_recv, w_side_recv,
    t_send, t_recv, s_send, s_recv, local_sem,
    *, line, pairs, members, tps,
):
    dp = lax.axis_index("dp")
    tp = lax.axis_index("tp")
    z, x = dp // pairs, dp % pairs
    size = line * pairs
    base = dp // members * members
    spot = dp % members
    token_rows = hidden.shape[0]
    feats = hidden.shape[1]
    depth = weight.shape[0]
    width = weight.shape[1]

    barrier = pltpu.get_barrier_semaphore()
    for k in range(1, size):
        pl.semaphore_signal(barrier, inc=1, device_id={"dp": (dp + k) % size}, device_id_type=MESH)
    for k in range(1, tps):
        pl.semaphore_signal(barrier, inc=1, device_id={"tp": (tp + k) % tps}, device_id_type=MESH)
    pl.semaphore_wait(barrier, size - 1 + tps - 1)

    half = tp // 2
    core = tp % 2
    mate = half * 2 + 1 - core
    across = (1 - half) * 2 + core
    side = z * pairs + 1 - x

    def feat_cols(owner):
        return pl.ds(pl.multiple_of(owner * feats, feats), feats)

    def weight_rows(zo, xo):
        return pl.ds(pl.multiple_of((zo * pairs + xo) * depth, depth), depth)

    def remote(src, dst, send, recv, where):
        return pltpu.make_async_remote_copy(
            src_ref=src, dst_ref=dst, send_sem=send, recv_sem=recv, device_id=where, device_id_type=MESH
        )

    def hidden_copy(n, src, owner, where):
        return remote(src, h_full.at[:, feat_cols(owner)], h_send.at[n], h_recv.at[n], where)

    def weight_copy(src, zo, sems, where):
        return remote(src, w_full.at[weight_rows(zo, x), :], sems.at[zo], w_recv.at[zo], where)

    def weight_aside(src, zo, xo):
        return remote(src, w_full.at[weight_rows(zo, xo), :], w_side.at[zo], w_side_recv.at[zo], {"dp": side})

    def onward(src, zo, up, down):
        if up:
            @pl.when(z < line - 1)
            def _():
                weight_copy(src, zo, w_up, {"dp": dp + pairs}).start()
        if down:
            @pl.when(z > 0)
            def _():
                weight_copy(src, zo, w_down, {"dp": dp - pairs}).start()
        weight_aside(src, zo, x).start()

    hidden_copy(0, hidden, tp, {"tp": across}).start()
    hidden_copy(1, hidden, tp, {"tp": mate}).start()
    onward(weight, z, True, True)
    h_own = pltpu.make_async_copy(hidden, h_full.at[:, feat_cols(tp)], local_sem.at[0])
    h_own.start()
    w_own = pltpu.make_async_copy(weight, w_full.at[weight_rows(z, x), :], local_sem.at[1])
    w_own.start()
    t_cols = teacher.shape[1] // members
    s_cols = width // members

    def part(k, n):
        return pl.ds(pl.multiple_of(k * n, n), n)

    own_rows = part(spot, token_rows)
    t_in = pltpu.make_async_copy(teacher.at[:, part(spot, t_cols)], t_stage, local_sem.at[2])
    t_in.start()

    def step(d, below):
        zo = z - d if below else z + d
        there = zo >= 0 if below else zo < line
        return zo, there

    def arrive(d):
        for below in (True, False):
            zo, there = step(d, below)

            @pl.when(there)
            def _():
                weight_copy(w_full.at[weight_rows(zo, x), :], zo, w_up, {"dp": dp}).wait_recv()
                onward(w_full.at[weight_rows(zo, x), :], zo, below, not below)

    def add(zo, xo, first=False):
        rows = 256 if token_rows % 256 == 0 else token_rows
        cols = 256 if width % 256 == 0 else width
        span = weight_rows(zo, xo)

        def tile(i, carry):
            at = part(i // (width // cols), rows)
            to = part(i % (width // cols), cols)
            term = jnp.dot(h_full[at, span], w_full[span, to], preferred_element_type=jnp.float32)
            total[at, to] = term if first else total[at, to] + term
            return carry

        lax.fori_loop(0, (token_rows // rows) * (width // cols), tile, 0)

    def add_mine(d):
        for below in (True, False):
            zo, there = step(d, below)

            @pl.when(there)
            def _():
                add(zo, x)

    def add_side(d):
        for below in (True, False) if d else (True,):
            zo, there = step(d, below)

            @pl.when(there)
            def _():
                weight_aside(w_full.at[weight_rows(zo, 1 - x), :], zo, 1 - x).wait_recv()
                add(zo, 1 - x)

    arrive(1)
    hidden_copy(0, hidden, across, {"tp": across}).wait_recv()
    hidden_copy(2, h_full.at[:, feat_cols(across)], across, {"tp": mate}).start()
    hidden_copy(1, hidden, mate, {"tp": mate}).wait_recv()
    h_own.wait()
    w_own.wait()
    far = (1 - half) * 2 + 1 - core
    hidden_copy(2, hidden, far, {"tp": mate}).wait_recv()
    h_out = pltpu.make_async_copy(h_full, hidden_out, local_sem.at[0])
    h_out.start()
    add(z, x, True)
    add_side(0)
    add_mine(1)
    for d in range(2, line):
        arrive(d)
        if d == line - 1:
            for k in range(1, members):
                to = (spot + k) % members
                remote(
                    teacher.at[:, part(to, t_cols)], teacher_out.at[own_rows, :], t_send.at[k], t_recv.at[k], {"dp": base + to}
                ).start()
        add_side(d - 1)
        add_mine(d)
    add_side(line - 1)

    s_loc[...] = total[...].astype(jnp.bfloat16)
    for k in range(1, members):
        to = (spot + k) % members
        remote(
            s_loc.at[:, part(to, s_cols)], student_out.at[own_rows, :], s_send.at[k], s_recv.at[k], {"dp": base + to}
        ).start()
    t_in.wait()
    t_out = pltpu.make_async_copy(t_stage, teacher_out.at[own_rows, :], local_sem.at[2])
    t_out.start()
    s_own = pltpu.make_async_copy(s_loc.at[:, part(spot, s_cols)], student_out.at[own_rows, :], local_sem.at[1])
    s_own.start()

    hidden_copy(0, hidden, tp, {"tp": across}).wait_send()
    hidden_copy(1, hidden, tp, {"tp": mate}).wait_send()
    hidden_copy(2, hidden, across, {"tp": mate}).wait_send()
    for d in range(line):
        for below in (True, False) if d else (True,):
            zo, there = step(d, below)

            @pl.when(jnp.logical_and(there, z < line - 1) if below else False)
            def _():
                weight_copy(weight, zo, w_up, {"dp": dp}).wait_send()

            @pl.when(jnp.logical_and(there, z > 0) if not below or d == 0 else False)
            def _():
                weight_copy(weight, zo, w_down, {"dp": dp}).wait_send()

            @pl.when(there)
            def _():
                weight_aside(weight, zo, x).wait_send()
    for k in range(1, members):
        source = (spot + members - k) % members
        from_rows = part(source, token_rows)
        t_copy = remote(
            teacher.at[:, part(spot, t_cols)], teacher_out.at[from_rows, :], t_send.at[k], t_recv.at[k], {"dp": base + source}
        )
        s_copy = remote(
            s_loc.at[:, part(spot, s_cols)], student_out.at[from_rows, :], s_send.at[k], s_recv.at[k], {"dp": base + source}
        )
        t_copy.wait()
        s_copy.wait()
    h_out.wait()
    t_out.wait()
    s_own.wait()


def gather_and_project(teacher_query, student_hidden, query_weight):
    tps, size = lax.axis_size("tp"), lax.axis_size("dp")
    members = size // NSEQ
    pairs = 2
    line = size // pairs
    rows, feats = student_hidden.shape
    depth, width = query_weight.shape
    dma = pltpu.SemaphoreType.DMA
    any_space = pl.BlockSpec(memory_space=pl.ANY)
    return pl.pallas_call(
        functools.partial(gather_body, line=line, pairs=pairs, members=members, tps=tps),
        in_specs=[any_space] * 3,
        out_specs=[any_space] * 3,
        out_shape=[
            jax.ShapeDtypeStruct((members * rows, teacher_query.shape[1] // members), jnp.bfloat16),
            jax.ShapeDtypeStruct((members * rows, width // members), jnp.bfloat16),
            jax.ShapeDtypeStruct((rows, tps * feats), jnp.bfloat16),
        ],
        scratch_shapes=[
            pltpu.VMEM((rows, tps * feats), jnp.bfloat16),
            pltpu.VMEM((size * depth, width), jnp.bfloat16),
            pltpu.VMEM((rows, width), jnp.float32),
            pltpu.VMEM((rows, width), jnp.bfloat16),
            pltpu.VMEM((rows, teacher_query.shape[1] // members), jnp.bfloat16),
            dma((3,)), dma((3,)), dma((line,)), dma((line,)), dma((line,)), dma((line,)), dma((line,)),
            dma((members,)), dma((members,)), dma((members,)), dma((members,)), dma((3,)),
        ],
        compiler_params=pltpu.CompilerParams(
            collective_id=0, has_side_effects=True, vmem_limit_bytes=60 * 1024 * 1024
        ),
        name="gather_and_project",
    )(teacher_query, student_hidden, query_weight)


def reduce_body(
    hidden, grad, out, h_all, g_all, own, x_out, x_in, z_out, z_in,
    g_send, g_recv, x_send, x_recv, z_send, z_recv, local_sem,
    *, line, pairs, members,
):
    dp = lax.axis_index("dp")
    z, x = dp // pairs, dp % pairs
    size = line * pairs
    base = dp // members * members
    spot = dp % members
    token_rows = h_all.shape[0]
    depth = out.shape[0]
    g_cols = grad.shape[1]
    tall = 256 if depth % 256 == 0 else depth

    barrier = pltpu.get_barrier_semaphore()
    for k in range(1, size):
        pl.semaphore_signal(barrier, inc=1, device_id={"dp": (dp + k) % size}, device_id_type=MESH)
    h_in = pltpu.make_async_copy(hidden, h_all, local_sem.at[0])
    h_in.start()
    pl.semaphore_wait(barrier, size - 1)

    def part(k, n):
        return pl.ds(pl.multiple_of(k * n, n), n)

    def remote(src, dst, send, recv, to):
        return pltpu.make_async_remote_copy(
            src_ref=src, dst_ref=dst, send_sem=send, recv_sem=recv, device_id={"dp": to}, device_id_type=MESH
        )

    def grad_copy(k, to):
        return remote(
            grad.at[part(to % members, token_rows), :], g_all.at[:, part(spot, g_cols)], g_send.at[k], g_recv.at[k], to
        )

    for k in range(1, members):
        grad_copy(k, base + (spot + k) % members).start()
    g_own = pltpu.make_async_copy(
        grad.at[part(spot, token_rows), :], g_all.at[:, part(spot, g_cols)], local_sem.at[1]
    )
    g_own.start()
    h_in.wait()
    g_own.wait()
    for k in range(1, members):
        grad_copy(k, base + (spot + members - k) % members).wait_recv()

    shifts = [line // 2] + [s for s in range(line - 1, 0, -1) if s != line // 2] + [0]

    def multiply(zo, xo, into):
        def tile(i, carry):
            at = pl.ds(pl.multiple_of((zo * pairs + xo) * depth + i * tall, tall), tall)
            term = lax.dot_general(
                h_all[:, at], g_all[...], (((0,), (0,)), ((), ())), preferred_element_type=jnp.float32
            )
            into[part(i, tall), :] = term.astype(into.dtype)
            return carry

        lax.fori_loop(0, depth // tall, tile, 0)

    def aside(n):
        return remote(x_out.at[n], x_in.at[n], x_send.at[n], x_recv.at[n], z * pairs + 1 - x)

    def along(s, zo):
        return remote(z_out.at[s], z_in.at[s], z_send.at[s], z_recv.at[s], zo * pairs + x)

    for n, s in enumerate(shifts):
        multiply((z + s) % line, 1 - x, x_out.at[n])
        aside(n).start()
    for n, s in enumerate(shifts):
        multiply((z + s) % line, x, own.at[n])
    for n, s in enumerate(shifts):
        aside(n).wait_recv()
        if s:
            z_out[s] = (own[n] + x_in[n].astype(jnp.float32)).astype(jnp.bfloat16)
            along(s, (z + s) % line).start()
        else:
            own[n] = own[n] + x_in[n].astype(jnp.float32)
    for s in shifts[:-1]:
        along(s, (z + s) % line).wait_recv()
    total = own[line - 1]
    for s in shifts[:-1]:
        total = total + z_in[s].astype(jnp.float32)
    out[...] = total

    for k in range(1, members):
        grad_copy(k, base + (spot + k) % members).wait_send()
    for n, s in enumerate(shifts):
        aside(n).wait_send()
        if s:
            along(s, (z + s) % line).wait_send()


def reduce_weight(hidden_full, grad):
    size = lax.axis_size("dp")
    members = size // NSEQ
    pairs = 2
    line = size // pairs
    rows, feats = hidden_full.shape
    width = grad.shape[1] * members
    depth = feats // size
    dma = pltpu.SemaphoreType.DMA
    any_space = pl.BlockSpec(memory_space=pl.ANY)
    return pl.pallas_call(
        functools.partial(reduce_body, line=line, pairs=pairs, members=members),
        in_specs=[any_space] * 2,
        out_specs=pl.BlockSpec(memory_space=pltpu.VMEM),
        out_shape=jax.ShapeDtypeStruct((depth, width), jnp.float32),
        scratch_shapes=[
            pltpu.VMEM((rows, feats), jnp.bfloat16),
            pltpu.VMEM((rows, width), jnp.bfloat16),
            pltpu.VMEM((line, depth, width), jnp.float32),
            pltpu.VMEM((line, depth, width), jnp.bfloat16),
            pltpu.VMEM((line, depth, width), jnp.bfloat16),
            pltpu.VMEM((line, depth, width), jnp.bfloat16),
            pltpu.VMEM((line, depth, width), jnp.bfloat16),
            dma((members,)), dma((members,)), dma((line,)), dma((line,)), dma((line,)), dma((line,)), dma((2,)),
        ],
        compiler_params=pltpu.CompilerParams(
            collective_id=1, has_side_effects=True, vmem_limit_bytes=60 * 1024 * 1024
        ),
        name="reduce_weight",
    )(hidden_full, grad)


def heads_of_one_sequence(teacher_query, student_hidden, query_weight):
    members = lax.axis_size("dp") // NSEQ
    mine = RHEADS // lax.axis_size("tp") // members
    groups = [[s * members + k for k in range(members)] for s in range(NSEQ)]
    teacher_all, student_all, hidden_full = gather_and_project(teacher_query, student_hidden, query_weight)
    rows_of = [0.0] * NSEQ
    kl, grad = relation(teacher_all, student_all, mine)
    for m in range(mine):
        for s in range(NSEQ):
            pairs = [(s * members + k, k * mine + m) for k in range(members)]
            rows_of[s] = rows_of[s] + lax.ppermute(kl[m], "dp", pairs)
    weight_grad = reduce_weight(hidden_full, grad)
    return jnp.concatenate(rows_of).reshape(1, NSEQ * SEQ), weight_grad


def local(teacher_query, student_hidden, query_weight):
    heads_here = RHEADS // lax.axis_size("tp")
    copies = lax.axis_size("dp") // heads_here
    if lax.axis_size("dp") % NSEQ == 0 and heads_here % (lax.axis_size("dp") // NSEQ) == 0:
        return heads_of_one_sequence(teacher_query, student_hidden, query_weight)
    rows = teacher_query.shape[0]
    teacher_width = teacher_query.shape[1] // heads_here
    hidden_full = lax.all_gather(student_hidden, "tp", axis=1, tiled=True)
    teacher_send = spread_heads(teacher_query, heads_here, copies)
    projected = jnp.dot(
        hidden_full,
        lax.all_gather(query_weight, "dp", axis=0, tiled=True),
        preferred_element_type=jnp.float32,
    )
    student_query = projected.astype(jnp.bfloat16)
    student_width = student_query.shape[1] // heads_here
    student_send = spread_heads(student_query, heads_here, copies)
    teacher_all, student_all = (
        lax.all_to_all(teacher_send, "dp", split_axis=1, concat_axis=0, tiled=True),
        lax.all_to_all(student_send, "dp", split_axis=1, concat_axis=0, tiled=True),
    )
    total_rows = teacher_all.shape[0]
    teacher_all = teacher_all.reshape(total_rows, teacher_width)
    student_all = student_all.reshape(total_rows, student_width)
    teacher_scale = teacher_width ** (-0.5)
    student_scale = student_width ** (-0.5)
    query_rows = SEQ // copies
    first_row = lax.axis_index("dp") % copies * query_rows
    block = min(512, query_rows)
    blocks_each = query_rows // block

    def relation_step(step, carry):
        kl_store, grad_store = carry
        sequence = step // blocks_each
        offset = step % blocks_each * block
        base = sequence * SEQ
        start = base + first_row + offset
        teacher_keys = lax.dynamic_slice_in_dim(teacher_all, base, SEQ, 0)
        student_keys = lax.dynamic_slice_in_dim(student_all, base, SEQ, 0)
        teacher_rows = lax.dynamic_slice_in_dim(teacher_all, start, block, 0)
        student_rows = lax.dynamic_slice_in_dim(student_all, start, block, 0)
        teacher_scores = (
            lax.dot_general(
                teacher_rows,
                teacher_keys,
                (((1,), (1,)), ((), ())),
                preferred_element_type=jnp.float32,
            )
            * teacher_scale
        )
        student_scores = (
            lax.dot_general(
                student_rows,
                student_keys,
                (((1,), (1,)), ((), ())),
                preferred_element_type=jnp.float32,
            )
            * student_scale
        )
        teacher_log = jax.nn.log_softmax(teacher_scores, axis=-1)
        student_log = jax.nn.log_softmax(student_scores, axis=-1)
        teacher_prob = jnp.exp(teacher_log)
        divergence = jnp.sum(teacher_prob * (teacher_log - student_log), axis=-1)
        score_grad = (jnp.exp(student_log) - teacher_prob).astype(jnp.bfloat16)
        key_part = (
            lax.dot_general(
                score_grad,
                student_rows,
                (((0,), (0,)), ((), ())),
                preferred_element_type=jnp.float32,
            )
            * student_scale
        )
        row_part = (
            jnp.dot(score_grad, student_keys, preferred_element_type=jnp.float32) * student_scale
        )
        seq_grad = lax.dynamic_slice_in_dim(grad_store, base, SEQ, 0)
        grad_store = lax.dynamic_update_slice_in_dim(grad_store, seq_grad + key_part, base, 0)
        current = lax.dynamic_slice_in_dim(grad_store, start, block, 0)
        grad_store = lax.dynamic_update_slice_in_dim(grad_store, current + row_part, start, 0)
        kl_store = lax.dynamic_update_slice_in_dim(
            kl_store, divergence, sequence * query_rows + offset, 0
        )
        return (kl_store, grad_store)

    kl_init = jnp.zeros((NSEQ * query_rows,), jnp.float32)
    grad_init = jnp.zeros((total_rows, student_width), jnp.float32)
    kl_store, grad_store = lax.fori_loop(0, NSEQ * blocks_each, relation_step, (kl_init, grad_init))
    returned = lax.all_to_all(
        grad_store.reshape(heads_here * copies, rows, student_width),
        "dp",
        split_axis=0,
        concat_axis=2,
        tiled=True,
    )
    summed = jnp.sum(returned.reshape(rows, heads_here, copies, student_width), axis=2)
    query_grad = summed.reshape(rows, heads_here * student_width).astype(jnp.bfloat16)
    weight_grad = lax.psum_scatter(
        lax.dot_general(
            hidden_full, query_grad, (((0,), (0,)), ((), ())), preferred_element_type=jnp.float32
        ),
        "dp",
        scatter_dimension=0,
        tiled=True,
    )
    return (kl_store.reshape(1, NSEQ * query_rows), weight_grad)


def solution(mesh):
    placed = (P("dp", "tp"), P("dp", "tp"), P("dp", "tp"))
    return jax.shard_map(
        local,
        mesh=mesh,
        in_specs=placed,
        out_specs=(P(("tp", "dp"), None), P("dp", "tp")),
        check_vma=False,
    )
```
